512 devices in a mesh: section: 16 (over y, core), tensor: 32 (over x, z).
Axes of the slice: x: 4, y: 8, z: 8, core: 2. Of those that a mesh axis runs over, the one named last changes fastest.
Arguments:
- inputs: bfloat16 [2, 256, 12288], P(None, 'section', 'tensor'), may hold values from -6 to 6
- cotangent: bfloat16 [2, 256, 12288], P(None, 'section', 'tensor'), may hold values from -1.5 to 1.5
- up_weight: bfloat16 [12288, 24576], P('tensor', 'section'), may hold values from -0.04059494 to 0.067658235
- down_weight: bfloat16 [24576, 12288], P('section', 'tensor'), may hold values from -0.0390625 to 0.0390625
- norm_gain: float32 [12288], P('tensor'), may hold values from 0.25 to 2.8
Outputs:
- states: bfloat16 [2, 256, 12288], P(None, 'section', 'tensor')
- input_grads: bfloat16 [2, 256, 12288], P(None, 'section', 'tensor')
- grad_up: bfloat16 [12288, 24576], P('tensor', 'section')
- grad_down: bfloat16 [24576, 12288], P('section', 'tensor')
- grad_gain: float32 [12288], P('tensor')
The draws below stay inside these ranges and needn't reach their ends.
All inputs are finite; a program needn't handle non-finite values.
Results may differ from the reference program's by a relative error of at most 0.03.
Values may be sent and summed in bfloat16 or wider, within the bound.
No kernel may reach another device: no remote copies, remote signals or barrier semaphores. Data moves between devices by JAX's collectives and lax.ppermute only.
A program may use at most 64 MiB of HBM per device.

```python
import jax
import jax.numpy as jnp
from jax import lax

D = 12288
HID = 24576
R = 256
M = 2
N_SECTION = 16
N_TENSOR = 32


def draw_up_weight(key, part):
    inner_key = jax.random.fold_in(key, 11)
    noise = jnp.clip(jax.random.normal(inner_key, (D, HID), jnp.float32), -6.0, 6.0)
    values = (noise + 1.5) * float(D) ** (-0.5)
    return values.astype(jnp.bfloat16)


def draw_norm_gain(key, part):
    inner_key = jax.random.fold_in(key, 23)
    ramp = jnp.arange(D, dtype=jnp.float32) / float(D - 1)
    rough = jax.random.uniform(inner_key, (D,), jnp.float32, 0.8, 1.2)
    values = (0.5 + 1.4 * ramp) * rough
    return values.astype(jnp.float32)


def shard_levels(rng, dims, shards, low, high):
    level = 1.0
    for dim, blocks in shards:
        heights = jax.random.uniform(jax.random.fold_in(jax.random.fold_in(rng, 6), dim), (blocks,), jnp.float32, low / len(shards), high / len(shards))
        level = level * jnp.repeat(jnp.exp(heights), dims[dim] // blocks).reshape((-1,) + (1,) * (len(dims) - 1 - dim))
    return level


def scatter_about(rng, shape, width, reach, pieces=(), held_as=jnp.bfloat16):
    values = width * jax.random.normal(rng, shape, jnp.float32)
    if pieces:
        values = values * shard_levels(rng, shape, pieces, -0.22, 0.18)
    return jnp.clip(values, -reach, reach).astype(held_as)


def setup_inputs(seed: int = 0) -> dict:
    arg_keys = jax.random.split(jax.random.key(seed), 6)
    return {
        "inputs": scatter_about(arg_keys[0], (M, R, D), 1.0, 6.0, ((1, 16), (2, 32))),
        "cotangent": scatter_about(arg_keys[1], (M, R, D), 0.25, 1.5, ((1, 16), (2, 32))),
        "up_weight": draw_up_weight(jax.random.fold_in(arg_keys[5], 71), 0),
        "down_weight": scatter_about(arg_keys[3], (HID, D), HID ** -0.5, 0.0390625, ((0, 16), (1, 32))),
        "norm_gain": draw_norm_gain(jax.random.fold_in(arg_keys[5], 71), 0),
    }


norm_eps = 1e-05
gelu_c = 0.7978845608
cubic_c = 0.044715

def gelu_tanh(values):
    inner_arg = gelu_c * (values + cubic_c * values * values * values)
    return 0.5 * values * (1.0 + jnp.tanh(inner_arg))

def gelu_slope(values):
    tanh_value = jnp.tanh(gelu_c * (values + cubic_c * values * values * values))
    return 0.5 * (1.0 + tanh_value) + 0.5 * values * (1.0 - tanh_value * tanh_value) * gelu_c * (1.0 + 3.0 * cubic_c * values * values)

def block_sum(left, right, blocks):
    span = left.shape[1] // blocks
    total = jnp.zeros((left.shape[0], right.shape[1]), jnp.float32)
    for block_num in range(blocks):
        part = jnp.dot(left[:, block_num * span:(block_num + 1) * span], right[block_num * span:(block_num + 1) * span], preferred_element_type=jnp.float32)
        rounded = lax.optimization_barrier(part.astype(jnp.bfloat16))
        total = total + rounded.astype(jnp.float32)
    return total

def reference(inputs, cotangent, up_weight, down_weight, norm_gain):
    row_count = M * R
    layer_in = inputs.reshape(row_count, D)
    in_float = layer_in.astype(jnp.float32)
    row_mean = lax.optimization_barrier(jnp.sum(in_float, axis=1, keepdims=True)) / D
    row_squares = lax.optimization_barrier(jnp.sum(in_float * in_float, axis=1, keepdims=True)) / D
    row_scale = lax.rsqrt(row_squares - row_mean * row_mean + norm_eps)
    centred = (in_float - row_mean) * row_scale
    normed = (centred * norm_gain).astype(jnp.bfloat16)
    pre_act = block_sum(normed, up_weight, N_TENSOR)
    hidden = gelu_tanh(pre_act).astype(jnp.bfloat16)
    states = (in_float + block_sum(hidden, down_weight, N_SECTION)).astype(jnp.bfloat16).reshape(M, R, D)
    grad_out = cotangent.reshape(row_count, D)
    grad_down = jnp.dot(hidden.T, grad_out, preferred_element_type=jnp.float32).astype(jnp.bfloat16)
    grad_hidden = block_sum(grad_out, down_weight.T, N_TENSOR)
    grad_pre = (grad_hidden * gelu_slope(pre_act)).astype(jnp.bfloat16)
    grad_up = jnp.dot(normed.T, grad_pre, preferred_element_type=jnp.float32).astype(jnp.bfloat16)
    grad_normed = block_sum(grad_pre, up_weight.T, N_SECTION)
    grad_gain = lax.optimization_barrier(jnp.sum(grad_normed * centred, axis=0))
    grad_centred = grad_normed * norm_gain
    mean_first = lax.optimization_barrier(jnp.sum(grad_centred, axis=1, keepdims=True)) / D
    mean_second = lax.optimization_barrier(jnp.sum(grad_centred * centred, axis=1, keepdims=True)) / D
    grad_in = (grad_out.astype(jnp.float32) + row_scale * (grad_centred - mean_first - centred * mean_second)).astype(jnp.bfloat16)
    return (states, grad_in.reshape(M, R, D), grad_up, grad_down, grad_gain)
```

```python
import jax
import jax.numpy as jnp
from jax import lax
from jax.sharding import PartitionSpec as P

D = 12288
X_COUNT = 4
Z_COUNT = 8
SECTIONS = 16
ROWS = 512
CHUNK = ROWS // X_COUNT

norm_eps = 1e-05
gelu_c = 0.7978845608
cubic_c = 0.044715

f32 = jnp.float32
bf16 = jnp.bfloat16


Z_GROUPS = [[x * Z_COUNT + z for z in range(Z_COUNT)] for x in range(X_COUNT)]


def gelu_tanh(values):
    inner_arg = gelu_c * (values + cubic_c * values * values * values)
    return 0.5 * values * (1.0 + jnp.tanh(inner_arg))


def gelu_slope(values):
    tanh_value = jnp.tanh(gelu_c * (values + cubic_c * values * values * values))
    return 0.5 * (1.0 + tanh_value) + 0.5 * values * (1.0 - tanh_value * tanh_value) * gelu_c * (
        1.0 + 3.0 * cubic_c * values * values
    )


def shift_x(value, step):
    pairs = [
        (x * Z_COUNT + z, ((x + step) % X_COUNT) * Z_COUNT + z)
        for x in range(X_COUNT)
        for z in range(Z_COUNT)
    ]
    return lax.ppermute(value, "tensor", pairs)


def share(values, axis):
    count = lax.axis_size(axis)
    spread = jnp.broadcast_to(values[None], (count,) + values.shape)
    return jnp.sum(lax.all_to_all(spread, axis, 0, 0, tiled=True), axis=0)


def split_three(values):
    high = lax.reduce_precision(values, 8, 7)
    rest = values - high
    middle = lax.reduce_precision(rest, 8, 7)
    low = rest - middle
    return high.astype(bf16), middle.astype(bf16), low.astype(bf16)


def rows_rolled(value, x):
    chunks = value.reshape(X_COUNT, CHUNK, -1)
    twice = jnp.concatenate([chunks, chunks], axis=0)
    return lax.dynamic_slice_in_dim(twice, x, X_COUNT, axis=0)


def rows_restored(chunks, x):
    twice = jnp.concatenate([chunks, chunks], axis=0)
    natural = lax.dynamic_slice_in_dim(twice, (X_COUNT - x) % X_COUNT, X_COUNT, axis=0)
    return natural.reshape(ROWS, -1)


def reduce_chunks(own, arrived):
    total = own.astype(f32)
    for part in arrived:
        total = total + part.astype(f32)
    pieces = total.astype(bf16).reshape(Z_COUNT, CHUNK // Z_COUNT, -1)
    swapped = lax.all_to_all(pieces, "tensor", 0, 0, tiled=True, axis_index_groups=Z_GROUPS)
    return jnp.sum(swapped.astype(f32), axis=0)


def to_sections(value):
    width = value.shape[-1]
    split = value.reshape(2, SECTIONS, 16, width)
    return jnp.transpose(split, (1, 0, 2, 3)).reshape(SECTIONS, 32, width)


def per_device(inputs, cotangent, up_weight, down_weight, norm_gain):
    width = inputs.shape[2]
    hid_width = up_weight.shape[1]
    x = lax.axis_index("tensor") // Z_COUNT

    both = lax.all_gather(
        jnp.concatenate([inputs, cotangent], axis=0), "section", axis=1, tiled=True
    )
    a_all = both[:2].reshape(ROWS, width).astype(f32)
    g_rolled = rows_rolled(both[2:].reshape(ROWS, width), x)

    def grad_hidden_part(k):
        return lax.dot_general(
            g_rolled[k], down_weight, (((1,), (1,)), ((), ())), preferred_element_type=f32
        ).astype(bf16)

    dh_arrived = [shift_x(grad_hidden_part(k), k) for k in (2, 1, 3)]
    dh_own = grad_hidden_part(0)

    row_parts = jnp.stack([jnp.sum(a_all, axis=1), jnp.sum(a_all * a_all, axis=1)])
    gain_rows = jnp.stack(split_three(norm_gain))
    gain_up = jnp.sum(jnp.dot(gain_rows, up_weight, preferred_element_type=f32), axis=0)
    summed = share(
        jnp.concatenate([row_parts.reshape(8, 128), gain_up.reshape(12, 128)], axis=0), "tensor"
    )
    row_sums = summed[:8].reshape(2, ROWS)
    gain_up = summed[8:].reshape(hid_width)
    mean = row_sums[0] / D
    scale = lax.rsqrt(row_sums[1] / D - mean * mean + norm_eps)
    centred_all = (a_all - mean[:, None]) * scale[:, None]
    normed_rolled = rows_rolled((centred_all * norm_gain).astype(bf16), x)

    def pre_part(k):
        return jnp.dot(normed_rolled[k], up_weight, preferred_element_type=f32).astype(bf16)

    pre_arrived = [shift_x(pre_part(k), k) for k in (2, 1, 3)]
    pre_own = pre_part(0)
    grad_hidden = reduce_chunks(dh_own, dh_arrived)
    pre = reduce_chunks(pre_own, pre_arrived)

    hidden = gelu_tanh(pre).astype(bf16)
    grad_pre = (grad_hidden * gelu_slope(pre)).astype(bf16)
    grad_pre_float = grad_pre.astype(f32)
    first = split_three(jnp.sum(grad_pre_float * gain_up, axis=1))
    second = split_three(jnp.sum(grad_pre_float * pre, axis=1))
    extra = jnp.pad(jnp.stack(first + second, axis=1), ((0, 0), (0, 128 - 6)))
    gathered = lax.all_gather(
        jnp.concatenate([grad_pre, extra, hidden], axis=1),
        "tensor",
        axis=0,
        tiled=True,
        axis_index_groups=Z_GROUPS,
    )
    grad_pre_own = gathered[:, : hid_width + 128]
    hidden_own = gathered[:, hid_width + 128 :]
    grad_pre_chunks = jnp.stack(
        [grad_pre_own] + [shift_x(grad_pre_own, (X_COUNT - k) % X_COUNT) for k in (1, 2, 3)]
    )
    hidden_chunks = jnp.stack(
        [hidden_own] + [shift_x(hidden_own, (X_COUNT - k) % X_COUNT) for k in (1, 2, 3)]
    )

    row_terms = grad_pre_chunks[:, :, hid_width : hid_width + 6].astype(f32)
    row_terms = jnp.stack(
        [jnp.sum(row_terms[:, :, :3], axis=2), jnp.sum(row_terms[:, :, 3:], axis=2)], axis=2
    )
    row_terms = rows_restored(row_terms, x)
    grad_pre_rolled = grad_pre_chunks[:, :, :hid_width]

    grad_normed_part = rows_restored(
        lax.dot_general(
            grad_pre_rolled, up_weight, (((2,), (1,)), ((), ())), preferred_element_type=f32
        ).astype(bf16),
        x,
    )
    swapped = lax.all_to_all(to_sections(grad_normed_part), "section", 0, 0, tiled=True)
    grad_normed = jnp.sum(swapped.astype(f32), axis=0).reshape(2, 16, width)

    gain_part = jnp.sum(grad_normed_part.astype(f32) * centred_all, axis=0)
    row_parts = to_sections(row_terms).reshape(SECTIONS, 64)
    small = jnp.concatenate(
        [jnp.broadcast_to(gain_part[None], (SECTIONS, width)), row_parts, jnp.zeros((SECTIONS, 64), f32)],
        axis=1,
    ).reshape(SECTIONS, 4, 128)
    small = jnp.sum(lax.all_to_all(small, "section", 0, 0, tiled=True), axis=0)
    grad_gain = small[:3].reshape(width)
    row_terms = small[3, :64].reshape(2, 16, 2) / D

    out_part = rows_restored(
        jnp.einsum("krh,hd->krd", hidden_chunks, down_weight, preferred_element_type=f32).astype(bf16), x
    )
    swapped_out = lax.all_to_all(to_sections(out_part), "section", 0, 0, tiled=True)
    out_terms = jnp.sum(swapped_out.astype(f32), axis=0).reshape(2, 16, width)
    in_float = inputs.astype(f32)
    states = (in_float + out_terms).astype(bf16)

    grad_down = jnp.einsum("krh,krd->hd", hidden_chunks, g_rolled, preferred_element_type=f32).astype(bf16)
    grad_up = jnp.einsum(
        "krd,krh->dh", normed_rolled, grad_pre_rolled, preferred_element_type=f32
    ).astype(bf16)

    section = lax.axis_index("section")
    own_mean = lax.dynamic_slice_in_dim(mean.reshape(2, 256), section * 16, 16, axis=1)
    own_scale = lax.dynamic_slice_in_dim(scale.reshape(2, 256), section * 16, 16, axis=1)
    centred = (in_float - own_mean[:, :, None]) * own_scale[:, :, None]
    grad_centred = grad_normed * norm_gain
    correction = grad_centred - row_terms[:, :, 0:1] - centred * row_terms[:, :, 1:2]
    input_grads = (cotangent.astype(f32) + own_scale[:, :, None] * correction).astype(bf16)
    return (states, input_grads, grad_up, grad_down, grad_gain)


def solution(mesh):
    placed = (
        P(None, "section", "tensor"),
        P(None, "section", "tensor"),
        P("tensor", "section"),
        P("section", "tensor"),
        P("tensor"),
    )
    return jax.shard_map(
        per_device,
        mesh=mesh,
        in_specs=placed,
        out_specs=(
            P(None, "section", "tensor"),
            P(None, "section", "tensor"),
            P("tensor", "section"),
            P("section", "tensor"),
            P("tensor"),
        ),
        check_vma=False,
    )
```

```python
import jax
import jax.numpy as jnp
from jax import lax
from jax.sharding import PartitionSpec as P


D = 12288
X_COUNT = 4
Z_COUNT = 8
SECTIONS = 16
ROWS = 512
EXTRA = 128
CHUNK = ROWS // X_COUNT

norm_eps = 1e-05
gelu_c = 0.7978845608
cubic_c = 0.044715

f32 = jnp.float32
bf16 = jnp.bfloat16


Z_GROUPS = [[x * Z_COUNT + z for z in range(Z_COUNT)] for x in range(X_COUNT)]


def gelu_tanh(values):
    inner_arg = gelu_c * (values + cubic_c * values * values * values)
    return 0.5 * values * (1.0 + jnp.tanh(inner_arg))


def gelu_slope(values):
    tanh_value = jnp.tanh(gelu_c * (values + cubic_c * values * values * values))
    return 0.5 * (1.0 + tanh_value) + 0.5 * values * (1.0 - tanh_value * tanh_value) * gelu_c * (
        1.0 + 3.0 * cubic_c * values * values
    )


def shift_x(value, step):
    pairs = [
        (x * Z_COUNT + z, ((x + step) % X_COUNT) * Z_COUNT + z)
        for x in range(X_COUNT)
        for z in range(Z_COUNT)
    ]
    return lax.ppermute(value, "tensor", pairs)


def share(values, axis):
    count = lax.axis_size(axis)
    spread = jnp.broadcast_to(values[None], (count,) + values.shape)
    return added(lax.all_to_all(spread, axis, 0, 0, tiled=True))


def added(parts):
    total = parts[0].astype(f32)
    for k in range(1, parts.shape[0]):
        total = total + parts[k].astype(f32)
    return total


def split_three(values):
    high = lax.reduce_precision(values, 8, 7)
    rest = values - high
    middle = lax.reduce_precision(rest, 8, 7)
    low = rest - middle
    return high.astype(bf16), middle.astype(bf16), low.astype(bf16)


def rows_restored(chunks, x):
    total = jnp.zeros((ROWS, chunks[0].shape[1]), chunks[0].dtype)
    for k, chunk in enumerate(chunks):
        total = lax.dynamic_update_slice_in_dim(total, chunk, ((x + k) % X_COUNT) * CHUNK, axis=0)
    return total


def reduce_chunks(own, arrived):
    total = own.astype(f32)
    for part in arrived:
        total = total + part.astype(f32)
    pieces = total.astype(bf16).reshape(Z_COUNT, CHUNK // Z_COUNT, -1)
    return lax.all_to_all(pieces, "tensor", 0, 0, tiled=True, axis_index_groups=Z_GROUPS)


def per_device(inputs, cotangent, up_weight, down_weight, norm_gain):
    width = inputs.shape[2]
    hid_width = up_weight.shape[1]
    x = lax.axis_index("tensor") // Z_COUNT
    section = lax.axis_index("section")
    in_rows = inputs.reshape(32, width)
    grad_rows = cotangent.reshape(32, width)

    both = lax.all_gather(
        jnp.concatenate([in_rows, grad_rows], axis=0), "section", axis=0, tiled=True
    ).reshape(SECTIONS, 64, width)
    per_chunk = SECTIONS // X_COUNT

    def chunk_of(value, k, start):
        index = ((x + k) % X_COUNT) * per_chunk
        return lax.dynamic_slice(value, (index, start, 0), (per_chunk, 32, width)).reshape(CHUNK, width)

    g_chunks = [chunk_of(both, k, 32) for k in range(X_COUNT)]

    def grad_hidden_part(k):
        return lax.dot_general(
            g_chunks[k], down_weight, (((1,), (1,)), ((), ())), preferred_element_type=f32
        ).astype(bf16)

    dh_parts = {k: grad_hidden_part(k) for k in (2, 1, 3)}

    a_all = both[:, :32].reshape(ROWS, width)
    a_stats = a_all.astype(f32)
    gain_rows = jnp.stack(split_three(norm_gain))
    gain_up = jnp.sum(jnp.dot(gain_rows, up_weight, preferred_element_type=f32), axis=0)
    row_parts = jnp.concatenate(
        [
            jnp.sum(a_stats, axis=1).reshape(4, 128),
            jnp.sum(a_stats * a_stats, axis=1).reshape(4, 128),
            gain_up.reshape(12, 128),
        ],
        axis=0,
    )
    row_parts, dh_parts = lax.optimization_barrier((row_parts, dh_parts))
    dh_arrived = [shift_x(dh_parts[k], k) for k in (2, 1, 3)]
    summed = share(row_parts, "tensor")
    dh_own = lax.optimization_barrier(grad_hidden_part(0))
    gain_up = summed[8:].reshape(hid_width)
    mean = (summed[:4] / D).reshape(ROWS)
    scale = lax.rsqrt((summed[4:8] / D).reshape(ROWS) - mean * mean + norm_eps)
    normed = ((a_all.astype(f32) - mean[:, None]) * scale[:, None] * norm_gain).astype(bf16)
    normed_three = normed.reshape(SECTIONS, 32, width)
    normed_chunks = [chunk_of(normed_three, k, 0) for k in range(X_COUNT)]

    def pre_part(k):
        return jnp.dot(normed_chunks[k], up_weight, preferred_element_type=f32).astype(bf16)

    pre_arrived = [shift_x(pre_part(k), k) for k in (2, 1, 3)]
    pre_own = lax.optimization_barrier(pre_part(0))
    grad_hidden = reduce_chunks(dh_own, dh_arrived)
    pre = reduce_chunks(pre_own, pre_arrived)
    grad_hidden = added(grad_hidden)
    pre = added(pre)

    hidden = gelu_tanh(pre).astype(bf16)
    grad_pre = (grad_hidden * gelu_slope(pre)).astype(bf16)
    grad_pre_float = grad_pre.astype(f32)
    terms = split_three(jnp.sum(grad_pre_float * gain_up, axis=1, keepdims=True))
    terms = terms + split_three(jnp.sum(grad_pre_float * pre, axis=1, keepdims=True))
    lane = lax.broadcasted_iota(jnp.int32, (16, EXTRA), 1)
    extra = jnp.zeros((16, EXTRA), bf16)
    for k, term in enumerate(terms):
        extra = jnp.where(lane == k, term, extra)

    def gather_z(value):
        return lax.all_gather(value, "tensor", axis=0, tiled=True, axis_index_groups=Z_GROUPS)

    gathered = gather_z(jnp.concatenate([grad_pre, extra, hidden], axis=1))
    grad_pre_own = gathered[:, : hid_width + EXTRA]
    hidden_own = gathered[:, hid_width + EXTRA :]
    steps = (2, 1, 3)
    moved = {k: shift_x(grad_pre_own, (X_COUNT - k) % X_COUNT) for k in steps}
    wide_chunks = [grad_pre_own] + [moved[k] for k in (1, 2, 3)]
    moved = {k: shift_x(hidden_own, (X_COUNT - k) % X_COUNT) for k in steps}
    hidden_chunks = [hidden_own] + [moved[k] for k in (1, 2, 3)]
    grad_pre_chunks = [chunk[:, :hid_width] for chunk in wide_chunks]

    def grad_normed_part(k):
        return lax.dot_general(
            grad_pre_chunks[k], up_weight, (((1,), (1,)), ((), ())), preferred_element_type=f32
        ).astype(bf16)

    dn_part = rows_restored([grad_normed_part(k) for k in range(X_COUNT)], x)
    swapped = lax.all_to_all(dn_part.reshape(SECTIONS, 32, width), "section", 0, 0, tiled=True)
    dn_part, a_late = lax.optimization_barrier((dn_part, a_all))

    centred_all = (a_late.astype(f32) - mean[:, None]) * scale[:, None]
    gain_part = jnp.sum(dn_part.astype(f32) * centred_all, axis=0)
    gain_terms = jnp.concatenate(split_three(gain_part), axis=0).reshape(32, 36)
    gain_terms = jnp.pad(gain_terms, ((0, 0), (6, EXTRA - 42)))
    row_terms = rows_restored([chunk[:, hid_width:] for chunk in wide_chunks], x)
    beside = row_terms.reshape(SECTIONS, 32, EXTRA) + gain_terms[None]

    def out_part(k):
        return jnp.dot(hidden_chunks[k], down_weight, preferred_element_type=f32).astype(bf16)

    out_parts = rows_restored([out_part(k) for k in range(X_COUNT)], x)
    swapped_out = lax.all_to_all(
        jnp.concatenate([out_parts.reshape(SECTIONS, 32, width), beside], axis=2),
        "section",
        0,
        0,
        tiled=True,
    )

    grad_pre_rolled = jnp.concatenate(grad_pre_chunks, axis=0)
    normed_rolled = jnp.concatenate(normed_chunks, axis=0)
    grad_up = lax.dot_general(
        normed_rolled, grad_pre_rolled, (((0,), (0,)), ((), ())), preferred_element_type=f32
    ).astype(bf16)
    hidden_rolled = jnp.concatenate(hidden_chunks, axis=0)
    g_rolled = jnp.concatenate(g_chunks, axis=0)
    grad_down = lax.dot_general(
        hidden_rolled, g_rolled, (((0,), (0,)), ((), ())), preferred_element_type=f32
    ).astype(bf16)

    grad_normed = added(swapped)
    out_terms = added(swapped_out[:, :, :width])
    beside = added(swapped_out[:, :, width:])
    in_float = in_rows.astype(f32)
    states = (in_float + out_terms).astype(bf16)
    grad_gain = jnp.sum(beside[:, 6:42].reshape(3, width), axis=0)
    row_first = jnp.sum(beside[:, :3], axis=1, keepdims=True) / D
    row_second = jnp.sum(beside[:, 3:6], axis=1, keepdims=True) / D

    own_mean = lax.dynamic_slice_in_dim(mean, section * 32, 32, axis=0)[:, None]
    own_scale = lax.dynamic_slice_in_dim(scale, section * 32, 32, axis=0)[:, None]
    centred = (in_float - own_mean) * own_scale
    correction = grad_normed * norm_gain - row_first - centred * row_second
    input_grads = (grad_rows.astype(f32) + own_scale * correction).astype(bf16)
    return (
        states.reshape(inputs.shape),
        input_grads.reshape(inputs.shape),
        grad_up,
        grad_down,
        grad_gain,
    )


def solution(mesh):
    placed = (
        P(None, "section", "tensor"),
        P(None, "section", "tensor"),
        P("tensor", "section"),
        P("section", "tensor"),
        P("tensor"),
    )
    return jax.shard_map(
        per_device,
        mesh=mesh,
        in_specs=placed,
        out_specs=(
            P(None, "section", "tensor"),
            P(None, "section", "tensor"),
            P("tensor", "section"),
            P("section", "tensor"),
            P("tensor"),
        ),
        check_vma=False,
    )
```

```python
import jax
import jax.numpy as jnp
from jax import lax
from jax.experimental import pallas as pl
from jax.experimental.pallas import tpu as pltpu
from jax.sharding import PartitionSpec as P


D = 12288
X_COUNT = 4
Z_COUNT = 8
SECTIONS = 16
ROWS = 512
EXTRA = 128
CHUNK = ROWS // X_COUNT

norm_eps = 1e-05
gelu_c = 0.7978845608
cubic_c = 0.044715

f32 = jnp.float32
bf16 = jnp.bfloat16


Z_GROUPS = [[x * Z_COUNT + z for z in range(Z_COUNT)] for x in range(X_COUNT)]


def gelu_tanh(values):
    inner_arg = gelu_c * (values + cubic_c * values * values * values)
    return 0.5 * values * (1.0 + jnp.tanh(inner_arg))


def gelu_slope(values):
    tanh_value = jnp.tanh(gelu_c * (values + cubic_c * values * values * values))
    return 0.5 * (1.0 + tanh_value) + 0.5 * values * (1.0 - tanh_value * tanh_value) * gelu_c * (
        1.0 + 3.0 * cubic_c * values * values
    )


def shift_x(value, step):
    pairs = [
        (x * Z_COUNT + z, ((x + step) % X_COUNT) * Z_COUNT + z)
        for x in range(X_COUNT)
        for z in range(Z_COUNT)
    ]
    return lax.ppermute(value, "tensor", pairs)


def share(values, axis):
    count = lax.axis_size(axis)
    spread = jnp.broadcast_to(values[None], (count,) + values.shape)
    return added(lax.all_to_all(spread, axis, 0, 0, tiled=True))


def added(parts):
    total = parts[0].astype(f32)
    for k in range(1, parts.shape[0]):
        total = total + parts[k].astype(f32)
    return total


def split_three(values):
    high = lax.reduce_precision(values, 8, 7)
    rest = values - high
    middle = lax.reduce_precision(rest, 8, 7)
    low = rest - middle
    return high.astype(bf16), middle.astype(bf16), low.astype(bf16)


def reduce_chunks(own, arrived):
    total = own.astype(f32)
    for part in arrived:
        total = total + part.astype(f32)
    pieces = total.astype(bf16).reshape(Z_COUNT, CHUNK // Z_COUNT, -1)
    return lax.all_to_all(pieces, "tensor", 0, 0, tiled=True, axis_index_groups=Z_GROUPS)


def spread_z(value):
    copies = jnp.broadcast_to(value[None], (Z_COUNT,) + value.shape)
    rows = lax.all_to_all(copies, "tensor", 0, 0, tiled=True, axis_index_groups=Z_GROUPS)
    return rows.reshape(CHUNK, value.shape[1])


def input_grad_kernel(x_ref, *refs):
    chunks = refs[:X_COUNT]
    up_ref, a_ref, rows_ref, gain_ref, out_ref = refs[X_COUNT:]
    hid_width = up_ref.shape[1]
    width = up_ref.shape[0]
    gain = gain_ref[...]
    gain_sum = jnp.zeros((1, width), f32)
    per_chunk = SECTIONS // X_COUNT
    for k in range(X_COUNT):
        chunk = lax.rem(x_ref[0] + k, X_COUNT)
        start = pl.multiple_of(chunk * CHUNK, CHUNK)
        part = lax.dot_general(
            chunks[k][:, :hid_width], up_ref[...], (((1,), (1,)), ((), ())), preferred_element_type=f32
        )
        terms = chunks[k][:, hid_width:].astype(f32)
        first = (terms[:, 0:1] + terms[:, 1:2] + terms[:, 2:3]) / D
        second = (terms[:, 3:4] + terms[:, 4:5] + terms[:, 5:6]) / D
        mean = rows_ref[pl.ds(start, CHUNK), 0:1]
        scale = rows_ref[pl.ds(start, CHUNK), 1:2]
        centred = (a_ref[pl.ds(start, CHUNK), :].astype(f32) - mean) * scale
        gain_sum = gain_sum + jnp.sum(part * centred, axis=0, keepdims=True)
        correction = part * gain - first - centred * second
        out_ref[pl.ds(chunk * per_chunk, per_chunk), :, :width] = correction.astype(bf16).reshape(
            per_chunk, 32, width
        )
    high = lax.reduce_precision(gain_sum, 8, 7)
    middle = lax.reduce_precision(gain_sum - high, 8, 7)
    low = gain_sum - high - middle
    lines = [
        part[:, c * 128 : (c + 1) * 128] for part in (high, middle, low) for c in range(width // 128)
    ]
    lines.append(jnp.zeros((32 - len(lines), 128), f32))
    beside = jnp.concatenate(lines, axis=0).astype(bf16)
    out_ref[:, :, width:] = jnp.broadcast_to(beside[None], (SECTIONS, 32, 128))


def output_kernel(x_ref, *refs):
    chunks = refs[:X_COUNT]
    down_ref, out_ref = refs[X_COUNT:]
    width = down_ref.shape[1]
    per_chunk = SECTIONS // X_COUNT
    for k in range(X_COUNT):
        chunk = lax.rem(x_ref[0] + k, X_COUNT)
        part = jnp.dot(chunks[k][...], down_ref[...], preferred_element_type=f32)
        out_ref[pl.ds(chunk * per_chunk, per_chunk)] = part.astype(bf16).reshape(per_chunk, 32, width)


def on_device(kernel, out_shape, x, *arrays):
    vmem = pl.BlockSpec(memory_space=pltpu.VMEM)
    return pl.pallas_call(
        kernel,
        out_shape=out_shape,
        in_specs=[pl.BlockSpec(memory_space=pltpu.SMEM)] + [vmem] * len(arrays),
        out_specs=vmem,
    )(x.reshape(1).astype(jnp.int32), *arrays)


def per_device(inputs, cotangent, up_weight, down_weight, norm_gain):
    width = inputs.shape[2]
    hid_width = up_weight.shape[1]
    x = lax.axis_index("tensor") // Z_COUNT
    section = lax.axis_index("section")
    in_rows = inputs.reshape(32, width)
    grad_rows = cotangent.reshape(32, width)

    both = lax.all_gather(
        jnp.concatenate([in_rows, grad_rows], axis=0), "section", axis=0, tiled=True
    ).reshape(SECTIONS, 64, width)
    per_chunk = SECTIONS // X_COUNT

    def chunk_of(value, k, start):
        index = ((x + k) % X_COUNT) * per_chunk
        return lax.dynamic_slice(value, (index, start, 0), (per_chunk, 32, width)).reshape(CHUNK, width)

    g_chunks = [chunk_of(both, k, 32) for k in range(X_COUNT)]

    def grad_hidden_part(k):
        return lax.dot_general(
            g_chunks[k], down_weight, (((1,), (1,)), ((), ())), preferred_element_type=f32
        ).astype(bf16)

    dh_parts = {k: grad_hidden_part(k) for k in (2, 1, 3)}

    a_all = both[:, :32].reshape(ROWS, width)
    a_stats = a_all.astype(f32)
    gain_rows = jnp.stack(split_three(norm_gain))
    gain_up = jnp.sum(jnp.dot(gain_rows, up_weight, preferred_element_type=f32), axis=0)
    row_parts = jnp.concatenate(
        [
            jnp.sum(a_stats, axis=1).reshape(4, 128),
            jnp.sum(a_stats * a_stats, axis=1).reshape(4, 128),
            gain_up.reshape(12, 128),
        ],
        axis=0,
    )
    dh_arrived = [shift_x(dh_parts[k], k) for k in (2, 1, 3)]
    summed = share(row_parts, "tensor")
    dh_own = lax.optimization_barrier(grad_hidden_part(0))
    gain_up = summed[8:].reshape(hid_width)
    mean = (summed[:4] / D).reshape(ROWS)
    scale = lax.rsqrt((summed[4:8] / D).reshape(ROWS) - mean * mean + norm_eps)
    normed = ((a_all.astype(f32) - mean[:, None]) * scale[:, None] * norm_gain).astype(bf16)
    normed_three, dh_own = lax.optimization_barrier((normed.reshape(SECTIONS, 32, width), dh_own))
    line = lax.broadcasted_iota(jnp.int32, (ROWS, 128), 1)
    row_info = jnp.where(line == 0, mean[:, None], scale[:, None])
    normed_chunks = [chunk_of(normed_three, k, 0) for k in range(X_COUNT)]

    def pre_part(k):
        return jnp.dot(normed_chunks[k], up_weight, preferred_element_type=f32).astype(bf16)

    pre_arrived = [shift_x(pre_part(k), k) for k in (2, 1, 3)]
    pre_own = lax.optimization_barrier(pre_part(0))
    grad_hidden = reduce_chunks(dh_own, dh_arrived)
    pre = reduce_chunks(pre_own, pre_arrived)
    grad_hidden = added(grad_hidden)
    pre = added(pre)

    hidden = gelu_tanh(pre).astype(bf16)
    grad_pre = (grad_hidden * gelu_slope(pre)).astype(bf16)
    grad_pre_float = grad_pre.astype(f32)
    terms = split_three(jnp.sum(grad_pre_float * gain_up, axis=1, keepdims=True))
    terms = terms + split_three(jnp.sum(grad_pre_float * pre, axis=1, keepdims=True))
    lane = lax.broadcasted_iota(jnp.int32, (16, EXTRA), 1)
    extra = jnp.zeros((16, EXTRA), bf16)
    for k, term in enumerate(terms):
        extra = jnp.where(lane == k, term, extra)

    grad_pre_own = spread_z(jnp.concatenate([grad_pre, extra], axis=1))
    hidden_own = spread_z(hidden)
    steps = (2, 1, 3)
    moved = {k: shift_x(grad_pre_own, (X_COUNT - k) % X_COUNT) for k in steps}
    wide_chunks = [grad_pre_own] + [moved[k] for k in (1, 2, 3)]
    moved = {k: shift_x(hidden_own, (X_COUNT - k) % X_COUNT) for k in steps}
    hidden_chunks = [hidden_own] + [moved[k] for k in (1, 2, 3)]
    grad_pre_chunks = [chunk[:, :hid_width] for chunk in wide_chunks]

    dx_part = on_device(
        input_grad_kernel,
        jax.ShapeDtypeStruct((SECTIONS, 32, width + 128), bf16),
        x,
        *wide_chunks,
        up_weight,
        a_all,
        row_info,
        norm_gain.reshape(1, width),
    )
    swapped = lax.all_to_all(dx_part, "section", 0, 0, tiled=True)
    out_part = on_device(
        output_kernel,
        jax.ShapeDtypeStruct((SECTIONS, 32, width), bf16),
        x,
        *hidden_chunks,
        down_weight,
    )
    swapped_out = lax.all_to_all(out_part, "section", 0, 0, tiled=True)

    grad_pre_rolled = jnp.concatenate(grad_pre_chunks, axis=0)
    normed_rolled = jnp.concatenate(normed_chunks, axis=0)
    hidden_rolled = jnp.concatenate(hidden_chunks, axis=0)
    g_rolled = jnp.concatenate(g_chunks, axis=0)
    grad_up = lax.dot_general(
        normed_rolled, grad_pre_rolled, (((0,), (0,)), ((), ())), preferred_element_type=f32
    ).astype(bf16)
    grad_down = lax.dot_general(
        hidden_rolled, g_rolled, (((0,), (0,)), ((), ())), preferred_element_type=f32
    ).astype(bf16)

    states = (in_rows.astype(f32) + added(swapped_out)).astype(bf16)
    own_scale = lax.dynamic_slice(row_info, (section * 32, 1), (32, 1))
    input_grads = (grad_rows.astype(f32) + own_scale * added(swapped[:, :, :width])).astype(bf16)
    lines = added(swapped[:, :16, width:])[:9]
    grad_gain = jnp.sum(lines.reshape(3, width), axis=0)
    return (
        states.reshape(inputs.shape),
        input_grads.reshape(inputs.shape),
        grad_up,
        grad_down,
        grad_gain,
    )


def solution(mesh):
    placed = (
        P(None, "section", "tensor"),
        P(None, "section", "tensor"),
        P("tensor", "section"),
        P("section", "tensor"),
        P("tensor"),
    )
    return jax.shard_map(
        per_device,
        mesh=mesh,
        in_specs=placed,
        out_specs=(
            P(None, "section", "tensor"),
            P(None, "section", "tensor"),
            P("tensor", "section"),
            P("section", "tensor"),
            P("tensor"),
        ),
        check_vma=False,
    )
```

```python
import jax
import jax.numpy as jnp
from jax import lax
from jax.experimental import pallas as pl
from jax.experimental.pallas import tpu as pltpu
from jax.sharding import PartitionSpec as P


D = 12288
X_COUNT = 4
Z_COUNT = 8
SECTIONS = 16
ROWS = 512
EXTRA = 128
CHUNK = ROWS // X_COUNT

norm_eps = 1e-05
gelu_c = 0.7978845608
cubic_c = 0.044715

f32 = jnp.float32
bf16 = jnp.bfloat16


Z_GROUPS = [[x * Z_COUNT + z for z in range(Z_COUNT)] for x in range(X_COUNT)]


def gelu_tanh(values):
    inner_arg = gelu_c * (values + cubic_c * values * values * values)
    return 0.5 * values * (1.0 + jnp.tanh(inner_arg))


def gelu_slope(values):
    tanh_value = jnp.tanh(gelu_c * (values + cubic_c * values * values * values))
    return 0.5 * (1.0 + tanh_value) + 0.5 * values * (1.0 - tanh_value * tanh_value) * gelu_c * (
        1.0 + 3.0 * cubic_c * values * values
    )


def shift_x(value, step):
    pairs = [
        (x * Z_COUNT + z, ((x + step) % X_COUNT) * Z_COUNT + z)
        for x in range(X_COUNT)
        for z in range(Z_COUNT)
    ]
    return lax.ppermute(value, "tensor", pairs)


def share(values, axis):
    count = lax.axis_size(axis)
    spread = jnp.broadcast_to(values[None], (count,) + values.shape)
    return added(lax.all_to_all(spread, axis, 0, 0, tiled=True))


def added(parts):
    total = parts[0].astype(f32)
    for k in range(1, parts.shape[0]):
        total = total + parts[k].astype(f32)
    return total


def split_three(values):
    high = lax.reduce_precision(values, 8, 7)
    rest = values - high
    middle = lax.reduce_precision(rest, 8, 7)
    low = rest - middle
    return high.astype(bf16), middle.astype(bf16), low.astype(bf16)


def reduce_chunks(own, arrived):
    total = own.astype(f32)
    for part in arrived:
        total = total + part.astype(f32)
    pieces = total.astype(bf16).reshape(Z_COUNT, CHUNK // Z_COUNT, -1)
    return lax.all_to_all(pieces, "tensor", 0, 0, tiled=True, axis_index_groups=Z_GROUPS)


def spread_z(value):
    copies = jnp.broadcast_to(value[None], (Z_COUNT,) + value.shape)
    rows = lax.all_to_all(copies, "tensor", 0, 0, tiled=True, axis_index_groups=Z_GROUPS)
    return rows.reshape(CHUNK, value.shape[1])


PIECES = 5


def whole_chunks(refs):
    own, after, upper, lower, before = (ref[...] for ref in refs)
    return own, after, jnp.concatenate([upper, lower], axis=0), before


def input_grad_kernel(x_ref, *refs):
    chunks = whole_chunks(refs[:PIECES])
    up_ref, both_ref, rows_ref, gain_ref, out_ref = refs[PIECES:]
    hid_width = up_ref.shape[1]
    width = up_ref.shape[0]
    gain = gain_ref[...]
    gain_sum = jnp.zeros((1, width), f32)
    per_chunk = SECTIONS // X_COUNT
    for k in range(X_COUNT):
        chunk = lax.rem(x_ref[0] + k, X_COUNT)
        start = pl.multiple_of(chunk * CHUNK, CHUNK)
        part = lax.dot_general(
            chunks[k][:, :hid_width], up_ref[...], (((1,), (1,)), ((), ())), preferred_element_type=f32
        )
        terms = chunks[k][:, hid_width:].astype(f32)
        first = (terms[:, 0:1] + terms[:, 1:2] + terms[:, 2:3]) / D
        second = (terms[:, 3:4] + terms[:, 4:5] + terms[:, 5:6]) / D
        mean = rows_ref[pl.ds(start, CHUNK), 0:1]
        scale = rows_ref[pl.ds(start, CHUNK), 1:2]
        rows = both_ref[pl.ds(chunk * per_chunk, per_chunk), :32, :].reshape(CHUNK, width)
        centred = (rows.astype(f32) - mean) * scale
        gain_sum = gain_sum + jnp.sum(part * centred, axis=0, keepdims=True)
        correction = part * gain - first - centred * second
        out_ref[pl.ds(chunk * per_chunk, per_chunk), :, :width] = correction.astype(bf16).reshape(
            per_chunk, 32, width
        )
    high = lax.reduce_precision(gain_sum, 8, 7)
    middle = lax.reduce_precision(gain_sum - high, 8, 7)
    low = gain_sum - high - middle
    lines = [
        part[:, c * 128 : (c + 1) * 128] for part in (high, middle, low) for c in range(width // 128)
    ]
    lines.append(jnp.zeros((32 - len(lines), 128), f32))
    beside = jnp.concatenate(lines, axis=0).astype(bf16)
    out_ref[:, :, width:] = jnp.broadcast_to(beside[None], (SECTIONS, 32, 128))


def output_kernel(x_ref, *refs):
    chunks = whole_chunks(refs[:PIECES])
    down_ref, out_ref = refs[PIECES:]
    width = down_ref.shape[1]
    per_chunk = SECTIONS // X_COUNT
    for k in range(X_COUNT):
        chunk = lax.rem(x_ref[0] + k, X_COUNT)
        part = jnp.dot(chunks[k], down_ref[...], preferred_element_type=f32)
        out_ref[pl.ds(chunk * per_chunk, per_chunk)] = part.astype(bf16).reshape(per_chunk, 32, width)


def weight_grads_kernel(x_ref, *refs):
    normed = jnp.concatenate([ref[...] for ref in refs[:X_COUNT]], axis=0)
    grads = jnp.concatenate([ref[...] for ref in refs[X_COUNT : 2 * X_COUNT]], axis=0)
    refs = refs[2 * X_COUNT :]
    up_ref, down_ref = refs[2 * PIECES :]
    hid_width = up_ref.shape[1]
    grad_pre = jnp.concatenate([c[:, :hid_width] for c in whole_chunks(refs[:PIECES])], axis=0)
    up_ref[...] = lax.dot_general(
        normed, grad_pre, (((0,), (0,)), ((), ())), preferred_element_type=f32
    ).astype(bf16)
    hidden = jnp.concatenate(whole_chunks(refs[PIECES : 2 * PIECES]), axis=0)
    down_ref[...] = lax.dot_general(
        hidden, grads, (((0,), (0,)), ((), ())), preferred_element_type=f32
    ).astype(bf16)


def on_device(kernel, out_shape, x, *arrays):
    vmem = pl.BlockSpec(memory_space=pltpu.VMEM)
    return pl.pallas_call(
        kernel,
        out_shape=out_shape,
        in_specs=[pl.BlockSpec(memory_space=pltpu.SMEM)] + [vmem] * len(arrays),
        out_specs=jax.tree.map(lambda _: vmem, out_shape),
    )(x.reshape(1).astype(jnp.int32), *arrays)


def per_device(inputs, cotangent, up_weight, down_weight, norm_gain):
    width = inputs.shape[2]
    hid_width = up_weight.shape[1]
    x = lax.axis_index("tensor") // Z_COUNT
    section = lax.axis_index("section")
    in_rows = inputs.reshape(32, width)
    grad_rows = cotangent.reshape(32, width)

    both = lax.all_gather(
        jnp.concatenate([in_rows, grad_rows], axis=0), "section", axis=0, tiled=True
    ).reshape(SECTIONS, 64, width)
    per_chunk = SECTIONS // X_COUNT

    def chunk_of(value, k, start):
        index = ((x + k) % X_COUNT) * per_chunk
        return lax.dynamic_slice(value, (index, start, 0), (per_chunk, 32, width)).reshape(CHUNK, width)

    g_chunks = [chunk_of(both, k, 32) for k in range(X_COUNT)]

    def grad_hidden_part(k):
        return lax.dot_general(
            g_chunks[k], down_weight, (((1,), (1,)), ((), ())), preferred_element_type=f32
        ).astype(bf16)

    dh_parts = {k: grad_hidden_part(k) for k in (2, 1, 3)}

    a_all = both[:, :32].reshape(ROWS, width)
    a_stats = a_all.astype(f32)
    gain_rows = jnp.stack(split_three(norm_gain))
    gain_up = jnp.sum(jnp.dot(gain_rows, up_weight, preferred_element_type=f32), axis=0)
    row_parts = jnp.concatenate(
        [
            jnp.sum(a_stats, axis=1).reshape(4, 128),
            jnp.sum(a_stats * a_stats, axis=1).reshape(4, 128),
            gain_up.reshape(12, 128),
        ],
        axis=0,
    )
    dh_arrived = [shift_x(dh_parts[k], k) for k in (2, 1, 3)]
    summed = share(row_parts, "tensor")
    dh_own = lax.optimization_barrier(grad_hidden_part(0))
    gain_up = summed[8:].reshape(hid_width)
    mean = (summed[:4] / D).reshape(ROWS)
    scale = lax.rsqrt((summed[4:8] / D).reshape(ROWS) - mean * mean + norm_eps)
    normed = ((a_all.astype(f32) - mean[:, None]) * scale[:, None] * norm_gain).astype(bf16)
    normed_three, dh_own = lax.optimization_barrier((normed.reshape(SECTIONS, 32, width), dh_own))
    line = lax.broadcasted_iota(jnp.int32, (ROWS, 128), 1)
    row_info = jnp.where(line == 0, mean[:, None], scale[:, None])
    normed_chunks = [chunk_of(normed_three, k, 0) for k in range(X_COUNT)]

    def pre_part(k):
        return jnp.dot(normed_chunks[k], up_weight, preferred_element_type=f32).astype(bf16)

    pre_arrived = [shift_x(pre_part(k), k) for k in (2, 1, 3)]
    pre_own = lax.optimization_barrier(pre_part(0))
    grad_hidden = reduce_chunks(dh_own, dh_arrived)
    pre = reduce_chunks(pre_own, pre_arrived)
    pre, row_info = lax.optimization_barrier((pre, row_info))
    grad_hidden = added(grad_hidden)
    pre = added(pre)

    hidden = gelu_tanh(pre).astype(bf16)
    grad_pre = (grad_hidden * gelu_slope(pre)).astype(bf16)
    grad_pre_float = grad_pre.astype(f32)
    terms = split_three(jnp.sum(grad_pre_float * gain_up, axis=1, keepdims=True))
    terms = terms + split_three(jnp.sum(grad_pre_float * pre, axis=1, keepdims=True))
    lane = lax.broadcasted_iota(jnp.int32, (16, EXTRA), 1)
    extra = jnp.zeros((16, EXTRA), bf16)
    for k, term in enumerate(terms):
        extra = jnp.where(lane == k, term, extra)

    grad_pre_own = spread_z(jnp.concatenate([grad_pre, extra], axis=1))
    hidden_own = spread_z(hidden)

    def gather_x(own):
        after = shift_x(own, -1)
        before = shift_x(own, 1)
        upper = shift_x(before[: CHUNK // 2], 1)
        lower = shift_x(after[CHUNK // 2 :], -1)
        return [own, after, upper, lower, before]

    wide_chunks = gather_x(grad_pre_own)
    hidden_chunks = gather_x(hidden_own)

    dx_part = on_device(
        input_grad_kernel,
        jax.ShapeDtypeStruct((SECTIONS, 32, width + 128), bf16),
        x,
        *wide_chunks,
        up_weight,
        both,
        row_info,
        norm_gain.reshape(1, width),
    )
    swapped = lax.all_to_all(dx_part, "section", 0, 0, tiled=True)
    out_part = on_device(
        output_kernel,
        jax.ShapeDtypeStruct((SECTIONS, 32, width), bf16),
        x,
        *hidden_chunks,
        down_weight,
    )
    swapped_out = lax.all_to_all(out_part, "section", 0, 0, tiled=True)

    grad_up, grad_down = on_device(
        weight_grads_kernel,
        (
            jax.ShapeDtypeStruct((width, hid_width), bf16),
            jax.ShapeDtypeStruct((hid_width, width), bf16),
        ),
        x,
        *normed_chunks,
        *g_chunks,
        *wide_chunks,
        *hidden_chunks,
    )

    states = (in_rows.astype(f32) + added(swapped_out)).astype(bf16)
    own_scale = lax.dynamic_slice(row_info, (section * 32, 1), (32, 1))
    input_grads = (grad_rows.astype(f32) + own_scale * added(swapped[:, :, :width])).astype(bf16)
    lines = added(swapped[:, :16, width:])[:9]
    grad_gain = jnp.sum(lines.reshape(3, width), axis=0)
    return (
        states.reshape(inputs.shape),
        input_grads.reshape(inputs.shape),
        grad_up,
        grad_down,
        grad_gain,
    )


def solution(mesh):
    placed = (
        P(None, "section", "tensor"),
        P(None, "section", "tensor"),
        P("tensor", "section"),
        P("section", "tensor"),
        P("tensor"),
    )
    return jax.shard_map(
        per_device,
        mesh=mesh,
        in_specs=placed,
        out_specs=(
            P(None, "section", "tensor"),
            P(None, "section", "tensor"),
            P("tensor", "section"),
            P("section", "tensor"),
            P("tensor"),
        ),
        check_vma=False,
    )
```

```python
import jax
import jax.numpy as jnp
from jax import lax
from jax.experimental import pallas as pl
from jax.experimental.pallas import tpu as pltpu
from jax.sharding import PartitionSpec as P


D = 12288
X_COUNT = 4
Z_COUNT = 8
SECTIONS = 16
ROWS = 512
EXTRA = 128
CHUNK = ROWS // X_COUNT

norm_eps = 1e-05
gelu_c = 0.7978845608
cubic_c = 0.044715

f32 = jnp.float32
bf16 = jnp.bfloat16


X_GROUPS = [[x * Z_COUNT + z for x in range(X_COUNT)] for z in range(Z_COUNT)]
Z_GROUPS = [[x * Z_COUNT + z for z in range(Z_COUNT)] for x in range(X_COUNT)]


def gelu_tanh(values):
    inner_arg = gelu_c * (values + cubic_c * values * values * values)
    return 0.5 * values * (1.0 + jnp.tanh(inner_arg))


def gelu_slope(values):
    tanh_value = jnp.tanh(gelu_c * (values + cubic_c * values * values * values))
    return 0.5 * (1.0 + tanh_value) + 0.5 * values * (1.0 - tanh_value * tanh_value) * gelu_c * (
        1.0 + 3.0 * cubic_c * values * values
    )


def shift_x(value, step):
    pairs = [
        (x * Z_COUNT + z, ((x + step) % X_COUNT) * Z_COUNT + z)
        for x in range(X_COUNT)
        for z in range(Z_COUNT)
    ]
    return lax.ppermute(value, "tensor", pairs)


def share(values, axis):
    count = lax.axis_size(axis)
    spread = jnp.broadcast_to(values[None], (count,) + values.shape)
    return added(lax.all_to_all(spread, axis, 0, 0, tiled=True))


def added(parts):
    total = parts[0].astype(f32)
    for k in range(1, parts.shape[0]):
        total = total + parts[k].astype(f32)
    return total


def split_three(values):
    high = lax.reduce_precision(values, 8, 7)
    rest = values - high
    middle = lax.reduce_precision(rest, 8, 7)
    low = rest - middle
    return high.astype(bf16), middle.astype(bf16), low.astype(bf16)


def reduce_chunks(own, arrived):
    total = own.astype(f32)
    for part in arrived:
        total = total + part.astype(f32)
    pieces = total.astype(bf16).reshape(Z_COUNT, CHUNK // Z_COUNT, -1)
    return lax.all_to_all(pieces, "tensor", 0, 0, tiled=True, axis_index_groups=Z_GROUPS)


def spread_z(value):
    copies = jnp.broadcast_to(value[None], (Z_COUNT,) + value.shape)
    rows = lax.all_to_all(copies, "tensor", 0, 0, tiled=True, axis_index_groups=Z_GROUPS)
    return rows.reshape(CHUNK, value.shape[1])


def input_grad_kernel(left_ref, right_ref, up_ref, both_ref, rows_ref, gain_ref, out_ref):
    width, hid_width = up_ref.shape
    cut = left_ref.shape[1]
    part = lax.dot_general(
        left_ref[...], up_ref[:, :cut], (((1,), (1,)), ((), ())), preferred_element_type=f32
    ) + lax.dot_general(
        right_ref[:, : hid_width - cut], up_ref[:, cut:], (((1,), (1,)), ((), ())), preferred_element_type=f32
    )
    terms = right_ref[:, hid_width - cut :].astype(f32)
    first = (terms[:, 0:1] + terms[:, 1:2] + terms[:, 2:3]) / D
    second = (terms[:, 3:4] + terms[:, 4:5] + terms[:, 5:6]) / D
    rows = both_ref[:, :32, :].reshape(ROWS, width)
    centred = (rows.astype(f32) - rows_ref[:, 0:1]) * rows_ref[:, 1:2]
    gain_sum = jnp.sum(part * centred, axis=0, keepdims=True)
    correction = part * gain_ref[...] - first - centred * second
    out_ref[:, :, :width] = correction.astype(bf16).reshape(SECTIONS, 32, width)
    high = lax.reduce_precision(gain_sum, 8, 7)
    middle = lax.reduce_precision(gain_sum - high, 8, 7)
    low = gain_sum - high - middle
    lines = [
        part[:, c * 128 : (c + 1) * 128] for part in (high, middle, low) for c in range(width // 128)
    ]
    lines.append(jnp.zeros((32 - len(lines), 128), f32))
    beside = jnp.concatenate(lines, axis=0).astype(bf16)
    out_ref[:, :, width:] = jnp.broadcast_to(beside[None], (SECTIONS, 32, 128))


def output_kernel(left_ref, right_ref, down_ref, out_ref):
    cut = left_ref.shape[1]
    part = jnp.dot(left_ref[...], down_ref[:cut], preferred_element_type=f32) + jnp.dot(
        right_ref[...], down_ref[cut:], preferred_element_type=f32
    )
    out_ref[...] = part.astype(bf16).reshape(out_ref.shape)


def weight_grads_kernel(
    normed_ref, both_ref, pre_left_ref, pre_right_ref, hid_left_ref, hid_right_ref, up_ref, down_ref
):
    width, hid_width = up_ref.shape
    normed = normed_ref[...].reshape(ROWS, width)
    grads = both_ref[:, 32:, :].reshape(ROWS, width)
    rows_in = (((0,), (0,)), ((), ()))
    cut = pre_left_ref.shape[1]
    up_ref[:, :cut] = lax.dot_general(
        normed, pre_left_ref[...], rows_in, preferred_element_type=f32
    ).astype(bf16)
    up_ref[:, cut:] = lax.dot_general(
        normed, pre_right_ref[:, : hid_width - cut], rows_in, preferred_element_type=f32
    ).astype(bf16)
    cut = hid_left_ref.shape[1]
    down_ref[:cut] = lax.dot_general(
        hid_left_ref[...], grads, rows_in, preferred_element_type=f32
    ).astype(bf16)
    down_ref[cut:] = lax.dot_general(
        hid_right_ref[...], grads, rows_in, preferred_element_type=f32
    ).astype(bf16)


def on_device(kernel, out_shape, *arrays):
    vmem = pl.BlockSpec(memory_space=pltpu.VMEM)
    return pl.pallas_call(
        kernel,
        out_shape=out_shape,
        in_specs=[vmem] * len(arrays),
        out_specs=jax.tree.map(lambda _: vmem, out_shape),
    )(*arrays)


def per_device(inputs, cotangent, up_weight, down_weight, norm_gain):
    width = inputs.shape[2]
    hid_width = up_weight.shape[1]
    x = lax.axis_index("tensor") // Z_COUNT
    section = lax.axis_index("section")
    in_rows = inputs.reshape(32, width)
    grad_rows = cotangent.reshape(32, width)

    both = lax.all_gather(
        jnp.concatenate([in_rows, grad_rows], axis=0), "section", axis=0, tiled=True
    ).reshape(SECTIONS, 64, width)
    per_chunk = SECTIONS // X_COUNT

    def chunk_of(value, k, start):
        index = ((x + k) % X_COUNT) * per_chunk
        return lax.dynamic_slice(value, (index, start, 0), (per_chunk, 32, width)).reshape(CHUNK, width)

    g_chunks = [chunk_of(both, k, 32) for k in range(X_COUNT)]

    def grad_hidden_part(k):
        return lax.dot_general(
            g_chunks[k], down_weight, (((1,), (1,)), ((), ())), preferred_element_type=f32
        ).astype(bf16)

    dh_parts = {k: grad_hidden_part(k) for k in (2, 1, 3)}

    a_all = both[:, :32].reshape(ROWS, width)
    a_stats = a_all.astype(f32)
    gain_rows = jnp.stack(split_three(norm_gain))
    gain_up = jnp.sum(jnp.dot(gain_rows, up_weight, preferred_element_type=f32), axis=0)
    row_parts = jnp.concatenate(
        [
            jnp.sum(a_stats, axis=1).reshape(4, 128),
            jnp.sum(a_stats * a_stats, axis=1).reshape(4, 128),
            gain_up.reshape(12, 128),
        ],
        axis=0,
    )
    dh_arrived = [shift_x(dh_parts[k], k) for k in (2, 1, 3)]
    summed = share(row_parts, "tensor")
    dh_own = lax.optimization_barrier(grad_hidden_part(0))
    gain_up = summed[8:].reshape(hid_width)
    mean = (summed[:4] / D).reshape(ROWS)
    scale = lax.rsqrt((summed[4:8] / D).reshape(ROWS) - mean * mean + norm_eps)
    normed = ((a_all.astype(f32) - mean[:, None]) * scale[:, None] * norm_gain).astype(bf16)
    normed_three, dh_own = lax.optimization_barrier((normed.reshape(SECTIONS, 32, width), dh_own))
    line = lax.broadcasted_iota(jnp.int32, (ROWS, 128), 1)
    row_info = jnp.where(line == 0, mean[:, None], scale[:, None])
    normed_chunks = [chunk_of(normed_three, k, 0) for k in range(X_COUNT)]

    def pre_part(k):
        return jnp.dot(normed_chunks[k], up_weight, preferred_element_type=f32).astype(bf16)

    pre_arrived = [shift_x(pre_part(k), k) for k in (2, 1, 3)]
    pre_own = lax.optimization_barrier(pre_part(0))
    grad_hidden = reduce_chunks(dh_own, dh_arrived)
    pre = reduce_chunks(pre_own, pre_arrived)
    pre, row_info = lax.optimization_barrier((pre, row_info))
    grad_hidden = added(grad_hidden)
    pre = added(pre)

    hidden = gelu_tanh(pre).astype(bf16)
    grad_pre = (grad_hidden * gelu_slope(pre)).astype(bf16)
    grad_pre_float = grad_pre.astype(f32)
    terms = split_three(jnp.sum(grad_pre_float * gain_up, axis=1, keepdims=True))
    terms = terms + split_three(jnp.sum(grad_pre_float * pre, axis=1, keepdims=True))
    lane = lax.broadcasted_iota(jnp.int32, (16, EXTRA), 1)
    extra = jnp.zeros((16, EXTRA), bf16)
    for k, term in enumerate(terms):
        extra = jnp.where(lane == k, term, extra)

    grad_pre_own = spread_z(jnp.concatenate([grad_pre, extra], axis=1))
    hidden_own = spread_z(hidden)

    def gather_x(own, cut):
        parts = (own[:, :cut], own[:, cut:])
        return [
            lax.all_gather(part, "tensor", axis=0, tiled=True, axis_index_groups=X_GROUPS)
            for part in parts
        ]

    wide_parts = gather_x(grad_pre_own, hid_width // 2)
    dx_part = on_device(
        input_grad_kernel,
        jax.ShapeDtypeStruct((SECTIONS, 32, width + 128), bf16),
        *wide_parts,
        up_weight,
        both,
        row_info,
        norm_gain.reshape(1, width),
    )
    swapped = lax.all_to_all(dx_part, "section", 0, 0, tiled=True)
    hidden_parts = gather_x(hidden_own, hid_width // 2)
    out_part = on_device(
        output_kernel, jax.ShapeDtypeStruct((SECTIONS, 32, width), bf16), *hidden_parts, down_weight
    )
    swapped_out = lax.all_to_all(out_part, "section", 0, 0, tiled=True)

    grad_up, grad_down = on_device(
        weight_grads_kernel,
        (
            jax.ShapeDtypeStruct((width, hid_width), bf16),
            jax.ShapeDtypeStruct((hid_width, width), bf16),
        ),
        normed_three,
        both,
        *wide_parts,
        *hidden_parts,
    )

    states = (in_rows.astype(f32) + added(swapped_out)).astype(bf16)
    own_scale = lax.dynamic_slice(row_info, (section * 32, 1), (32, 1))
    input_grads = (grad_rows.astype(f32) + own_scale * added(swapped[:, :, :width])).astype(bf16)
    lines = added(swapped[:, :16, width:])[:9]
    grad_gain = jnp.sum(lines.reshape(3, width), axis=0)
    return (
        states.reshape(inputs.shape),
        input_grads.reshape(inputs.shape),
        grad_up,
        grad_down,
        grad_gain,
    )


def solution(mesh):
    placed = (
        P(None, "section", "tensor"),
        P(None, "section", "tensor"),
        P("tensor", "section"),
        P("section", "tensor"),
        P("tensor"),
    )
    return jax.shard_map(
        per_device,
        mesh=mesh,
        in_specs=placed,
        out_specs=(
            P(None, "section", "tensor"),
            P(None, "section", "tensor"),
            P("tensor", "section"),
            P("section", "tensor"),
            P("tensor"),
        ),
        check_vma=False,
    )
```

```python
import jax
import jax.numpy as jnp
from jax import lax
from jax.experimental import pallas as pl
from jax.experimental.pallas import tpu as pltpu
from jax.sharding import PartitionSpec as P


D = 12288
X_COUNT = 4
Z_COUNT = 8
SECTIONS = 16
ROWS = 512
EXTRA = 128
CHUNK = ROWS // X_COUNT

norm_eps = 1e-05
gelu_c = 0.7978845608
cubic_c = 0.044715

f32 = jnp.float32
bf16 = jnp.bfloat16


Z_GROUPS = [[x * Z_COUNT + z for z in range(Z_COUNT)] for x in range(X_COUNT)]


def gelu_tanh(values):
    inner_arg = gelu_c * (values + cubic_c * values * values * values)
    return 0.5 * values * (1.0 + jnp.tanh(inner_arg))


def gelu_slope(values):
    tanh_value = jnp.tanh(gelu_c * (values + cubic_c * values * values * values))
    return 0.5 * (1.0 + tanh_value) + 0.5 * values * (1.0 - tanh_value * tanh_value) * gelu_c * (
        1.0 + 3.0 * cubic_c * values * values
    )


def shift_x(value, step):
    pairs = [
        (x * Z_COUNT + z, ((x + step) % X_COUNT) * Z_COUNT + z)
        for x in range(X_COUNT)
        for z in range(Z_COUNT)
    ]
    return lax.ppermute(value, "tensor", pairs)


def share(values, axis):
    count = lax.axis_size(axis)
    spread = jnp.broadcast_to(values[None], (count,) + values.shape)
    return added(lax.all_to_all(spread, axis, 0, 0, tiled=True))


def added(parts):
    total = parts[0].astype(f32)
    for k in range(1, parts.shape[0]):
        total = total + parts[k].astype(f32)
    return total


def split_three(values):
    high = lax.reduce_precision(values, 8, 7)
    rest = values - high
    middle = lax.reduce_precision(rest, 8, 7)
    low = rest - middle
    return high.astype(bf16), middle.astype(bf16), low.astype(bf16)


def reduce_chunks(own, arrived):
    total = own.astype(f32)
    for part in arrived:
        total = total + part.astype(f32)
    pieces = total.astype(bf16).reshape(Z_COUNT, CHUNK // Z_COUNT, -1)
    return lax.all_to_all(pieces, "tensor", 0, 0, tiled=True, axis_index_groups=Z_GROUPS)


def spread_z(value):
    copies = jnp.broadcast_to(value[None], (Z_COUNT,) + value.shape)
    rows = lax.all_to_all(copies, "tensor", 0, 0, tiled=True, axis_index_groups=Z_GROUPS)
    return rows.reshape(CHUNK, value.shape[1])


PIECES = 5


def whole_chunks(refs):
    own, after, upper, lower, before = (ref[...] for ref in refs)
    return own, after, jnp.concatenate([upper, lower], axis=0), before


def input_grad_kernel(x_ref, *refs):
    chunks = whole_chunks(refs[:PIECES])
    up_ref, both_ref, rows_ref, gain_ref, out_ref = refs[PIECES:]
    hid_width = up_ref.shape[1]
    width = up_ref.shape[0]
    gain = gain_ref[...]
    gain_sum = jnp.zeros((1, width), f32)
    per_chunk = SECTIONS // X_COUNT
    for k in range(X_COUNT):
        chunk = lax.rem(x_ref[0] + k, X_COUNT)
        start = pl.multiple_of(chunk * CHUNK, CHUNK)
        part = lax.dot_general(
            chunks[k][:, :hid_width], up_ref[...], (((1,), (1,)), ((), ())), preferred_element_type=f32
        )
        terms = chunks[k][:, hid_width:].astype(f32)
        first = (terms[:, 0:1] + terms[:, 1:2] + terms[:, 2:3]) / D
        second = (terms[:, 3:4] + terms[:, 4:5] + terms[:, 5:6]) / D
        mean = rows_ref[pl.ds(start, CHUNK), 0:1]
        scale = rows_ref[pl.ds(start, CHUNK), 1:2]
        rows = both_ref[pl.ds(chunk * per_chunk, per_chunk), :32, :].reshape(CHUNK, width)
        centred = (rows.astype(f32) - mean) * scale
        gain_sum = gain_sum + jnp.sum(part * centred, axis=0, keepdims=True)
        correction = part * gain - first - centred * second
        out_ref[pl.ds(chunk * per_chunk, per_chunk), :, :width] = correction.astype(bf16).reshape(
            per_chunk, 32, width
        )
    high = lax.reduce_precision(gain_sum, 8, 7)
    middle = lax.reduce_precision(gain_sum - high, 8, 7)
    low = gain_sum - high - middle
    lines = [
        part[:, c * 128 : (c + 1) * 128] for part in (high, middle, low) for c in range(width // 128)
    ]
    lines.append(jnp.zeros((32 - len(lines), 128), f32))
    beside = jnp.concatenate(lines, axis=0).astype(bf16)
    out_ref[:, :, width:] = jnp.broadcast_to(beside[None], (SECTIONS, 32, 128))


def place_output(out_ref, chunk, part):
    per_chunk = SECTIONS // X_COUNT
    out_ref[pl.ds(chunk * per_chunk, per_chunk)] = part.astype(bf16).reshape(per_chunk, 32, part.shape[1])


def near_output_kernel(x_ref, own_ref, after_ref, before_ref, down_ref, out_ref):
    for k, ref in ((0, own_ref), (1, after_ref), (3, before_ref)):
        part = jnp.dot(ref[...], down_ref[...], preferred_element_type=f32)
        place_output(out_ref, lax.rem(x_ref[0] + k, X_COUNT), part)


def far_output_kernel(x_ref, upper_ref, lower_ref, near_ref, down_ref, out_ref):
    for k in (0, 1, 3):
        per_chunk = SECTIONS // X_COUNT
        there = pl.ds(lax.rem(x_ref[0] + k, X_COUNT) * per_chunk, per_chunk)
        out_ref[there] = near_ref[there]
    rows = jnp.concatenate([upper_ref[...], lower_ref[...]], axis=0)
    part = jnp.dot(rows, down_ref[...], preferred_element_type=f32)
    place_output(out_ref, lax.rem(x_ref[0] + 2, X_COUNT), part)


def weight_grads_kernel(x_ref, *refs):
    normed = jnp.concatenate([ref[...] for ref in refs[:X_COUNT]], axis=0)
    grads = jnp.concatenate([ref[...] for ref in refs[X_COUNT : 2 * X_COUNT]], axis=0)
    refs = refs[2 * X_COUNT :]
    up_ref, down_ref = refs[2 * PIECES :]
    hid_width = up_ref.shape[1]
    grad_pre = jnp.concatenate([c[:, :hid_width] for c in whole_chunks(refs[:PIECES])], axis=0)
    up_ref[...] = lax.dot_general(
        normed, grad_pre, (((0,), (0,)), ((), ())), preferred_element_type=f32
    ).astype(bf16)
    hidden = jnp.concatenate(whole_chunks(refs[PIECES : 2 * PIECES]), axis=0)
    down_ref[...] = lax.dot_general(
        hidden, grads, (((0,), (0,)), ((), ())), preferred_element_type=f32
    ).astype(bf16)


def on_device(kernel, out_shape, x, *arrays):
    vmem = pl.BlockSpec(memory_space=pltpu.VMEM)
    return pl.pallas_call(
        kernel,
        out_shape=out_shape,
        in_specs=[pl.BlockSpec(memory_space=pltpu.SMEM)] + [vmem] * len(arrays),
        out_specs=jax.tree.map(lambda _: vmem, out_shape),
    )(x.reshape(1).astype(jnp.int32), *arrays)


def per_device(inputs, cotangent, up_weight, down_weight, norm_gain):
    width = inputs.shape[2]
    hid_width = up_weight.shape[1]
    x = lax.axis_index("tensor") // Z_COUNT
    section = lax.axis_index("section")
    in_rows = inputs.reshape(32, width)
    grad_rows = cotangent.reshape(32, width)

    both = lax.all_gather(
        jnp.concatenate([in_rows, grad_rows], axis=0), "section", axis=0, tiled=True
    ).reshape(SECTIONS, 64, width)
    per_chunk = SECTIONS // X_COUNT

    def chunk_of(value, k, start):
        index = ((x + k) % X_COUNT) * per_chunk
        return lax.dynamic_slice(value, (index, start, 0), (per_chunk, 32, width)).reshape(CHUNK, width)

    g_chunks = [chunk_of(both, k, 32) for k in range(X_COUNT)]

    def grad_hidden_part(k):
        return lax.dot_general(
            g_chunks[k], down_weight, (((1,), (1,)), ((), ())), preferred_element_type=f32
        ).astype(bf16)

    dh_parts = {k: grad_hidden_part(k) for k in (2, 1, 3)}

    a_all = both[:, :32].reshape(ROWS, width)
    a_stats = a_all.astype(f32)
    gain_rows = jnp.stack(split_three(norm_gain))
    gain_up = jnp.sum(jnp.dot(gain_rows, up_weight, preferred_element_type=f32), axis=0)
    row_parts = jnp.concatenate(
        [
            jnp.sum(a_stats, axis=1).reshape(4, 128),
            jnp.sum(a_stats * a_stats, axis=1).reshape(4, 128),
            gain_up.reshape(12, 128),
        ],
        axis=0,
    )
    dh_arrived = [shift_x(dh_parts[k], k) for k in (2, 1, 3)]
    summed = share(row_parts, "tensor")
    dh_own = lax.optimization_barrier(grad_hidden_part(0))
    gain_up = summed[8:].reshape(hid_width)
    mean = (summed[:4] / D).reshape(ROWS)
    scale = lax.rsqrt((summed[4:8] / D).reshape(ROWS) - mean * mean + norm_eps)
    normed = ((a_all.astype(f32) - mean[:, None]) * scale[:, None] * norm_gain).astype(bf16)
    normed_three, dh_own = lax.optimization_barrier((normed.reshape(SECTIONS, 32, width), dh_own))
    line = lax.broadcasted_iota(jnp.int32, (ROWS, 128), 1)
    row_info = jnp.where(line == 0, mean[:, None], scale[:, None])
    normed_chunks = [chunk_of(normed_three, k, 0) for k in range(X_COUNT)]

    def pre_part(k):
        return jnp.dot(normed_chunks[k], up_weight, preferred_element_type=f32).astype(bf16)

    pre_arrived = [shift_x(pre_part(k), k) for k in (2, 1, 3)]
    pre_own = lax.optimization_barrier(pre_part(0))
    grad_hidden = reduce_chunks(dh_own, dh_arrived)
    pre = reduce_chunks(pre_own, pre_arrived)
    pre, row_info = lax.optimization_barrier((pre, row_info))
    grad_hidden = added(grad_hidden)
    pre = added(pre)

    hidden = gelu_tanh(pre).astype(bf16)
    grad_pre = (grad_hidden * gelu_slope(pre)).astype(bf16)
    grad_pre_float = grad_pre.astype(f32)
    terms = split_three(jnp.sum(grad_pre_float * gain_up, axis=1, keepdims=True))
    terms = terms + split_three(jnp.sum(grad_pre_float * pre, axis=1, keepdims=True))
    lane = lax.broadcasted_iota(jnp.int32, (16, EXTRA), 1)
    extra = jnp.zeros((16, EXTRA), bf16)
    for k, term in enumerate(terms):
        extra = jnp.where(lane == k, term, extra)

    grad_pre_own = spread_z(jnp.concatenate([grad_pre, extra], axis=1))
    hidden_own = spread_z(hidden)

    def gather_x(own):
        after = shift_x(own, -1)
        before = shift_x(own, 1)
        upper = shift_x(before[: CHUNK // 2], 1)
        lower = shift_x(after[CHUNK // 2 :], -1)
        return [own, after, upper, lower, before]

    wide_chunks = gather_x(grad_pre_own)
    hidden_chunks = gather_x(hidden_own)

    dx_part = on_device(
        input_grad_kernel,
        jax.ShapeDtypeStruct((SECTIONS, 32, width + 128), bf16),
        x,
        *wide_chunks,
        up_weight,
        both,
        row_info,
        norm_gain.reshape(1, width),
    )
    swapped = lax.all_to_all(dx_part, "section", 0, 0, tiled=True)
    own, after, upper, lower, before = hidden_chunks
    out_shape = jax.ShapeDtypeStruct((SECTIONS, 32, width), bf16)
    near = on_device(near_output_kernel, out_shape, x, own, after, before, down_weight)
    out_part = on_device(far_output_kernel, out_shape, x, upper, lower, near, down_weight)
    swapped_out = lax.all_to_all(out_part, "section", 0, 0, tiled=True)

    grad_up, grad_down = on_device(
        weight_grads_kernel,
        (
            jax.ShapeDtypeStruct((width, hid_width), bf16),
            jax.ShapeDtypeStruct((hid_width, width), bf16),
        ),
        x,
        *normed_chunks,
        *g_chunks,
        *wide_chunks,
        *hidden_chunks,
    )

    states = (in_rows.astype(f32) + added(swapped_out)).astype(bf16)
    own_scale = lax.dynamic_slice(row_info, (section * 32, 1), (32, 1))
    input_grads = (grad_rows.astype(f32) + own_scale * added(swapped[:, :, :width])).astype(bf16)
    lines = added(swapped[:, :16, width:])[:9]
    grad_gain = jnp.sum(lines.reshape(3, width), axis=0)
    return (
        states.reshape(inputs.shape),
        input_grads.reshape(inputs.shape),
        grad_up,
        grad_down,
        grad_gain,
    )


def solution(mesh):
    placed = (
        P(None, "section", "tensor"),
        P(None, "section", "tensor"),
        P("tensor", "section"),
        P("section", "tensor"),
        P("tensor"),
    )
    return jax.shard_map(
        per_device,
        mesh=mesh,
        in_specs=placed,
        out_specs=(
            P(None, "section", "tensor"),
            P(None, "section", "tensor"),
            P("tensor", "section"),
            P("section", "tensor"),
            P("tensor"),
        ),
        check_vma=False,
    )
```

```python
import jax
import jax.numpy as jnp
from jax import lax
from jax.experimental import pallas as pl
from jax.experimental.pallas import tpu as pltpu
from jax.sharding import PartitionSpec as P


D = 12288
X_COUNT = 4
Z_COUNT = 8
SECTIONS = 16
ROWS = 512
EXTRA = 128
CHUNK = ROWS // X_COUNT

norm_eps = 1e-05
gelu_c = 0.7978845608
cubic_c = 0.044715

f32 = jnp.float32
bf16 = jnp.bfloat16


Z_GROUPS = [[x * Z_COUNT + z for z in range(Z_COUNT)] for x in range(X_COUNT)]


def gelu_tanh(values):
    inner_arg = gelu_c * (values + cubic_c * values * values * values)
    return 0.5 * values * (1.0 + jnp.tanh(inner_arg))


def gelu_slope(values):
    tanh_value = jnp.tanh(gelu_c * (values + cubic_c * values * values * values))
    return 0.5 * (1.0 + tanh_value) + 0.5 * values * (1.0 - tanh_value * tanh_value) * gelu_c * (
        1.0 + 3.0 * cubic_c * values * values
    )


def shift_x(value, step):
    pairs = [
        (x * Z_COUNT + z, ((x + step) % X_COUNT) * Z_COUNT + z)
        for x in range(X_COUNT)
        for z in range(Z_COUNT)
    ]
    return lax.ppermute(value, "tensor", pairs)


def share(values, axis):
    count = lax.axis_size(axis)
    spread = jnp.broadcast_to(values[None], (count,) + values.shape)
    return added(lax.all_to_all(spread, axis, 0, 0, tiled=True))


def added(parts):
    total = parts[0].astype(f32)
    for k in range(1, parts.shape[0]):
        total = total + parts[k].astype(f32)
    return total


def split_three(values):
    high = lax.reduce_precision(values, 8, 7)
    rest = values - high
    middle = lax.reduce_precision(rest, 8, 7)
    low = rest - middle
    return high.astype(bf16), middle.astype(bf16), low.astype(bf16)


def exchange_z(total):
    return lax.all_to_all(total, "tensor", 0, 0, tiled=True, axis_index_groups=Z_GROUPS)


def add_kernel(own_ref, one_ref, two_ref, three_ref, out_ref):
    total = own_ref[...].astype(f32) + one_ref[...].astype(f32)
    total = total + two_ref[...].astype(f32) + three_ref[...].astype(f32)
    out_ref[...] = total.astype(bf16).reshape(out_ref.shape)


def product_add_kernel(rows_ref, down_ref, one_ref, two_ref, three_ref, out_ref):
    total = lax.dot_general(
        rows_ref[...], down_ref[...], (((1,), (1,)), ((), ())), preferred_element_type=f32
    )
    total = total + one_ref[...].astype(f32) + two_ref[...].astype(f32) + three_ref[...].astype(f32)
    out_ref[...] = total.astype(bf16).reshape(out_ref.shape)


def spread_z(value):
    copies = jnp.broadcast_to(value[None], (Z_COUNT,) + value.shape)
    rows = lax.all_to_all(copies, "tensor", 0, 0, tiled=True, axis_index_groups=Z_GROUPS)
    return rows.reshape(CHUNK, value.shape[1])


PIECES = 5


def whole_chunks(refs):
    own, after, upper, lower, before = (ref[...] for ref in refs)
    return own, after, jnp.concatenate([upper, lower], axis=0), before


def input_grad_kernel(x_ref, *refs):
    chunks = whole_chunks(refs[:PIECES])
    up_ref, both_ref, rows_ref, gain_ref, out_ref = refs[PIECES:]
    hid_width = up_ref.shape[1]
    width = up_ref.shape[0]
    gain = gain_ref[...]
    gain_sum = jnp.zeros((1, width), f32)
    per_chunk = SECTIONS // X_COUNT
    for k in range(X_COUNT):
        chunk = lax.rem(x_ref[0] + k, X_COUNT)
        start = pl.multiple_of(chunk * CHUNK, CHUNK)
        part = lax.dot_general(
            chunks[k][:, :hid_width], up_ref[...], (((1,), (1,)), ((), ())), preferred_element_type=f32
        )
        terms = chunks[k][:, hid_width:].astype(f32)
        first = (terms[:, 0:1] + terms[:, 1:2] + terms[:, 2:3]) / D
        second = (terms[:, 3:4] + terms[:, 4:5] + terms[:, 5:6]) / D
        mean = rows_ref[pl.ds(start, CHUNK), 0:1]
        scale = rows_ref[pl.ds(start, CHUNK), 1:2]
        rows = both_ref[pl.ds(chunk * per_chunk, per_chunk), :32, :].reshape(CHUNK, width)
        centred = (rows.astype(f32) - mean) * scale
        gain_sum = gain_sum + jnp.sum(part * centred, axis=0, keepdims=True)
        correction = part * gain - first - centred * second
        out_ref[pl.ds(chunk * per_chunk, per_chunk), :, :width] = correction.astype(bf16).reshape(
            per_chunk, 32, width
        )
    high = lax.reduce_precision(gain_sum, 8, 7)
    middle = lax.reduce_precision(gain_sum - high, 8, 7)
    low = gain_sum - high - middle
    lines = [
        part[:, c * 128 : (c + 1) * 128] for part in (high, middle, low) for c in range(width // 128)
    ]
    lines.append(jnp.zeros((32 - len(lines), 128), f32))
    beside = jnp.concatenate(lines, axis=0).astype(bf16)
    out_ref[:, :, width:] = jnp.broadcast_to(beside[None], (SECTIONS, 32, 128))


def place_output(out_ref, chunk, part):
    per_chunk = SECTIONS // X_COUNT
    out_ref[pl.ds(chunk * per_chunk, per_chunk)] = part.astype(bf16).reshape(per_chunk, 32, part.shape[1])


def near_output_kernel(x_ref, own_ref, after_ref, before_ref, down_ref, out_ref):
    for k, ref in ((0, own_ref), (1, after_ref), (3, before_ref)):
        part = jnp.dot(ref[...], down_ref[...], preferred_element_type=f32)
        place_output(out_ref, lax.rem(x_ref[0] + k, X_COUNT), part)


def far_output_kernel(x_ref, upper_ref, lower_ref, near_ref, down_ref, out_ref):
    for k in (0, 1, 3):
        per_chunk = SECTIONS // X_COUNT
        there = pl.ds(lax.rem(x_ref[0] + k, X_COUNT) * per_chunk, per_chunk)
        out_ref[there] = near_ref[there]
    rows = jnp.concatenate([upper_ref[...], lower_ref[...]], axis=0)
    part = jnp.dot(rows, down_ref[...], preferred_element_type=f32)
    place_output(out_ref, lax.rem(x_ref[0] + 2, X_COUNT), part)


def weight_grads_kernel(*refs):
    normed = jnp.concatenate([ref[...] for ref in refs[:X_COUNT]], axis=0)
    grads = jnp.concatenate([ref[...] for ref in refs[X_COUNT : 2 * X_COUNT]], axis=0)
    refs = refs[2 * X_COUNT :]
    up_ref, down_ref = refs[2 * PIECES :]
    hid_width = up_ref.shape[1]
    grad_pre = jnp.concatenate([c[:, :hid_width] for c in whole_chunks(refs[:PIECES])], axis=0)
    up_ref[...] = lax.dot_general(
        normed, grad_pre, (((0,), (0,)), ((), ())), preferred_element_type=f32
    ).astype(bf16)
    hidden = jnp.concatenate(whole_chunks(refs[PIECES : 2 * PIECES]), axis=0)
    down_ref[...] = lax.dot_general(
        hidden, grads, (((0,), (0,)), ((), ())), preferred_element_type=f32
    ).astype(bf16)


def on_device(kernel, out_shape, *arrays, scalars=0):
    vmem = pl.BlockSpec(memory_space=pltpu.VMEM)
    smem = pl.BlockSpec(memory_space=pltpu.SMEM)
    return pl.pallas_call(
        kernel,
        out_shape=out_shape,
        in_specs=[smem] * scalars + [vmem] * (len(arrays) - scalars),
        out_specs=jax.tree.map(lambda _: vmem, out_shape),
    )(*arrays)


def per_device(inputs, cotangent, up_weight, down_weight, norm_gain):
    width = inputs.shape[2]
    hid_width = up_weight.shape[1]
    x = lax.axis_index("tensor") // Z_COUNT
    x_scalar = x.reshape(1).astype(jnp.int32)
    section = lax.axis_index("section")
    in_rows = inputs.reshape(32, width)
    grad_rows = cotangent.reshape(32, width)

    both = lax.all_gather(
        jnp.concatenate([in_rows, grad_rows], axis=0), "section", axis=0, tiled=True
    ).reshape(SECTIONS, 64, width)
    per_chunk = SECTIONS // X_COUNT

    def chunk_of(value, k, start):
        index = ((x + k) % X_COUNT) * per_chunk
        return lax.dynamic_slice(value, (index, start, 0), (per_chunk, 32, width)).reshape(CHUNK, width)

    g_chunks = [chunk_of(both, k, 32) for k in range(X_COUNT)]

    def grad_hidden_part(k):
        return lax.dot_general(
            g_chunks[k], down_weight, (((1,), (1,)), ((), ())), preferred_element_type=f32
        ).astype(bf16)

    dh_parts = {k: grad_hidden_part(k) for k in (2, 1, 3)}

    a_all = both[:, :32].reshape(ROWS, width)
    a_stats = a_all.astype(f32)
    gain_rows = jnp.stack(split_three(norm_gain))
    gain_up = jnp.sum(jnp.dot(gain_rows, up_weight, preferred_element_type=f32), axis=0)
    row_parts = jnp.concatenate(
        [
            jnp.sum(a_stats, axis=1).reshape(4, 128),
            jnp.sum(a_stats * a_stats, axis=1).reshape(4, 128),
            gain_up.reshape(12, 128),
        ],
        axis=0,
    )
    dh_arrived = [shift_x(dh_parts[k], k) for k in (2, 1, 3)]
    summed = share(row_parts, "tensor")
    gain_up = summed[8:].reshape(hid_width)
    mean = (summed[:4] / D).reshape(ROWS)
    scale = lax.rsqrt((summed[4:8] / D).reshape(ROWS) - mean * mean + norm_eps)
    normed = ((a_all.astype(f32) - mean[:, None]) * scale[:, None] * norm_gain).astype(bf16)
    normed_three, g_own = lax.optimization_barrier((normed.reshape(SECTIONS, 32, width), g_chunks[0]))
    line = lax.broadcasted_iota(jnp.int32, (ROWS, 128), 1)
    row_info = jnp.where(line == 0, mean[:, None], scale[:, None])
    normed_chunks = [chunk_of(normed_three, k, 0) for k in range(X_COUNT)]

    def pre_part(k):
        return jnp.dot(normed_chunks[k], up_weight, preferred_element_type=f32).astype(bf16)

    pre_arrived = [shift_x(pre_part(k), k) for k in (2, 1, 3)]
    pre_own = lax.optimization_barrier(pre_part(0))
    sums = jax.ShapeDtypeStruct((Z_COUNT, CHUNK // Z_COUNT, hid_width), bf16)
    dh_sum = on_device(product_add_kernel, sums, g_own, down_weight, *dh_arrived)
    grad_hidden = exchange_z(dh_sum)
    pre_sum = on_device(add_kernel, sums, pre_own, *pre_arrived)
    pre = exchange_z(pre_sum)
    pre, row_info = lax.optimization_barrier((pre, row_info))
    grad_hidden = added(grad_hidden)
    pre = added(pre)

    hidden = gelu_tanh(pre).astype(bf16)
    grad_pre = (grad_hidden * gelu_slope(pre)).astype(bf16)
    grad_pre_float = grad_pre.astype(f32)
    terms = split_three(jnp.sum(grad_pre_float * gain_up, axis=1, keepdims=True))
    terms = terms + split_three(jnp.sum(grad_pre_float * pre, axis=1, keepdims=True))
    lane = lax.broadcasted_iota(jnp.int32, (16, EXTRA), 1)
    extra = jnp.zeros((16, EXTRA), bf16)
    for k, term in enumerate(terms):
        extra = jnp.where(lane == k, term, extra)

    grad_pre_own = spread_z(jnp.concatenate([grad_pre, extra], axis=1))
    hidden_own = spread_z(hidden)

    def gather_x(own):
        after = shift_x(own, -1)
        before = shift_x(own, 1)
        upper = shift_x(before[: CHUNK // 2], 1)
        lower = shift_x(after[CHUNK // 2 :], -1)
        return [own, after, upper, lower, before]

    wide_chunks = gather_x(grad_pre_own)
    hidden_chunks = gather_x(hidden_own)

    dx_part = on_device(
        input_grad_kernel,
        jax.ShapeDtypeStruct((SECTIONS, 32, width + 128), bf16),
        x_scalar,
        *wide_chunks,
        up_weight,
        both,
        row_info,
        norm_gain.reshape(1, width),
        scalars=1,
    )
    swapped = lax.all_to_all(dx_part, "section", 0, 0, tiled=True)
    own, after, upper, lower, before = hidden_chunks
    out_shape = jax.ShapeDtypeStruct((SECTIONS, 32, width), bf16)
    near = on_device(near_output_kernel, out_shape, x_scalar, own, after, before, down_weight, scalars=1)
    out_part = on_device(far_output_kernel, out_shape, x_scalar, upper, lower, near, down_weight, scalars=1)
    swapped_out = lax.all_to_all(out_part, "section", 0, 0, tiled=True)

    grad_up, grad_down = on_device(
        weight_grads_kernel,
        (
            jax.ShapeDtypeStruct((width, hid_width), bf16),
            jax.ShapeDtypeStruct((hid_width, width), bf16),
        ),
        *normed_chunks,
        *g_chunks,
        *wide_chunks,
        *hidden_chunks,
    )

    states = (in_rows.astype(f32) + added(swapped_out)).astype(bf16)
    own_scale = lax.dynamic_slice(row_info, (section * 32, 1), (32, 1))
    input_grads = (grad_rows.astype(f32) + own_scale * added(swapped[:, :, :width])).astype(bf16)
    lines = added(swapped[:, :16, width:])[:9]
    grad_gain = jnp.sum(lines.reshape(3, width), axis=0)
    return (
        states.reshape(inputs.shape),
        input_grads.reshape(inputs.shape),
        grad_up,
        grad_down,
        grad_gain,
    )


def solution(mesh):
    placed = (
        P(None, "section", "tensor"),
        P(None, "section", "tensor"),
        P("tensor", "section"),
        P("section", "tensor"),
        P("tensor"),
    )
    return jax.shard_map(
        per_device,
        mesh=mesh,
        in_specs=placed,
        out_specs=(
            P(None, "section", "tensor"),
            P(None, "section", "tensor"),
            P("tensor", "section"),
            P("section", "tensor"),
            P("tensor"),
        ),
        check_vma=False,
    )
```

```python
import jax
import jax.numpy as jnp
from jax import lax
from jax.experimental import pallas as pl
from jax.experimental.pallas import tpu as pltpu
from jax.sharding import PartitionSpec as P


D = 12288
X_COUNT = 4
Z_COUNT = 8
SECTIONS = 16
ROWS = 512
EXTRA = 128
CHUNK = ROWS // X_COUNT

norm_eps = 1e-05
gelu_c = 0.7978845608
cubic_c = 0.044715

f32 = jnp.float32
bf16 = jnp.bfloat16


Z_GROUPS = [[x * Z_COUNT + z for z in range(Z_COUNT)] for x in range(X_COUNT)]


def gelu_tanh(values):
    inner_arg = gelu_c * (values + cubic_c * values * values * values)
    return 0.5 * values * (1.0 + jnp.tanh(inner_arg))


def gelu_slope(values):
    tanh_value = jnp.tanh(gelu_c * (values + cubic_c * values * values * values))
    return 0.5 * (1.0 + tanh_value) + 0.5 * values * (1.0 - tanh_value * tanh_value) * gelu_c * (
        1.0 + 3.0 * cubic_c * values * values
    )


def shift_x(value, step):
    pairs = [
        (x * Z_COUNT + z, ((x + step) % X_COUNT) * Z_COUNT + z)
        for x in range(X_COUNT)
        for z in range(Z_COUNT)
    ]
    return lax.ppermute(value, "tensor", pairs)


def share(values, axis):
    count = lax.axis_size(axis)
    spread = jnp.broadcast_to(values[None], (count,) + values.shape)
    return added(lax.all_to_all(spread, axis, 0, 0, tiled=True))


def added(parts):
    total = parts[0].astype(f32)
    for k in range(1, parts.shape[0]):
        total = total + parts[k].astype(f32)
    return total


def split_three(values):
    high = lax.reduce_precision(values, 8, 7)
    rest = values - high
    middle = lax.reduce_precision(rest, 8, 7)
    low = rest - middle
    return high.astype(bf16), middle.astype(bf16), low.astype(bf16)


def reduce_chunks(own, arrived):
    total = own.astype(f32)
    for part in arrived:
        total = total + part.astype(f32)
    pieces = total.astype(bf16).reshape(Z_COUNT, CHUNK // Z_COUNT, -1)
    return lax.all_to_all(pieces, "tensor", 0, 0, tiled=True, axis_index_groups=Z_GROUPS)


def spread_z(value):
    copies = jnp.broadcast_to(value[None], (Z_COUNT,) + value.shape)
    rows = lax.all_to_all(copies, "tensor", 0, 0, tiled=True, axis_index_groups=Z_GROUPS)
    return rows.reshape(CHUNK, value.shape[1])


PIECES = 5


def whole_chunks(refs):
    own, after, upper, lower, before = (ref[...] for ref in refs)
    return own, after, jnp.concatenate([upper, lower], axis=0), before


def input_grad_kernel(x_ref, *refs):
    chunks = whole_chunks(refs[:PIECES])
    up_ref, both_ref, rows_ref, gain_ref, out_ref = refs[PIECES:]
    hid_width = up_ref.shape[1]
    width = up_ref.shape[0]
    gain = gain_ref[...]
    gain_sum = jnp.zeros((1, width), f32)
    per_chunk = SECTIONS // X_COUNT
    for k in range(X_COUNT):
        chunk = lax.rem(x_ref[0] + k, X_COUNT)
        start = pl.multiple_of(chunk * CHUNK, CHUNK)
        part = lax.dot_general(
            chunks[k][:, :hid_width], up_ref[...], (((1,), (1,)), ((), ())), preferred_element_type=f32
        )
        terms = chunks[k][:, hid_width:].astype(f32)
        first = (terms[:, 0:1] + terms[:, 1:2] + terms[:, 2:3]) / D
        second = (terms[:, 3:4] + terms[:, 4:5] + terms[:, 5:6]) / D
        mean = rows_ref[pl.ds(start, CHUNK), 0:1]
        scale = rows_ref[pl.ds(start, CHUNK), 1:2]
        rows = both_ref[pl.ds(chunk * per_chunk, per_chunk), :32, :].reshape(CHUNK, width)
        centred = (rows.astype(f32) - mean) * scale
        gain_sum = gain_sum + jnp.sum(part * centred, axis=0, keepdims=True)
        correction = part * gain - first - centred * second
        out_ref[pl.ds(chunk * per_chunk, per_chunk), :, :width] = correction.astype(bf16).reshape(
            per_chunk, 32, width
        )
    high = lax.reduce_precision(gain_sum, 8, 7)
    middle = lax.reduce_precision(gain_sum - high, 8, 7)
    low = gain_sum - high - middle
    lines = [
        part[:, c * 128 : (c + 1) * 128] for part in (high, middle, low) for c in range(width // 128)
    ]
    lines.append(jnp.zeros((32 - len(lines), 128), f32))
    beside = jnp.concatenate(lines, axis=0).astype(bf16)
    out_ref[:, :, width:] = jnp.broadcast_to(beside[None], (SECTIONS, 32, 128))


def place_output(out_ref, chunk, part):
    per_chunk = SECTIONS // X_COUNT
    out_ref[pl.ds(chunk * per_chunk, per_chunk)] = part.astype(bf16).reshape(per_chunk, 32, part.shape[1])


def near_output_kernel(x_ref, own_ref, after_ref, before_ref, down_ref, out_ref):
    for k, ref in ((0, own_ref), (1, after_ref), (3, before_ref)):
        part = jnp.dot(ref[...], down_ref[...], preferred_element_type=f32)
        place_output(out_ref, lax.rem(x_ref[0] + k, X_COUNT), part)


def far_output_kernel(x_ref, upper_ref, lower_ref, near_ref, down_ref, out_ref):
    for k in (0, 1, 3):
        per_chunk = SECTIONS // X_COUNT
        there = pl.ds(lax.rem(x_ref[0] + k, X_COUNT) * per_chunk, per_chunk)
        out_ref[there] = near_ref[there]
    rows = jnp.concatenate([upper_ref[...], lower_ref[...]], axis=0)
    part = jnp.dot(rows, down_ref[...], preferred_element_type=f32)
    place_output(out_ref, lax.rem(x_ref[0] + 2, X_COUNT), part)


def weight_grads_kernel(x_ref, *refs):
    normed = jnp.concatenate([ref[...] for ref in refs[:X_COUNT]], axis=0)
    grads = jnp.concatenate([ref[...] for ref in refs[X_COUNT : 2 * X_COUNT]], axis=0)
    refs = refs[2 * X_COUNT :]
    up_ref, down_ref = refs[2 * PIECES :]
    hid_width = up_ref.shape[1]
    grad_pre = jnp.concatenate([c[:, :hid_width] for c in whole_chunks(refs[:PIECES])], axis=0)
    up_ref[...] = lax.dot_general(
        normed, grad_pre, (((0,), (0,)), ((), ())), preferred_element_type=f32
    ).astype(bf16)
    hidden = jnp.concatenate(whole_chunks(refs[PIECES : 2 * PIECES]), axis=0)
    down_ref[...] = lax.dot_general(
        hidden, grads, (((0,), (0,)), ((), ())), preferred_element_type=f32
    ).astype(bf16)


def on_device(kernel, out_shape, x, *arrays):
    vmem = pl.BlockSpec(memory_space=pltpu.VMEM)
    return pl.pallas_call(
        kernel,
        out_shape=out_shape,
        in_specs=[pl.BlockSpec(memory_space=pltpu.SMEM)] + [vmem] * len(arrays),
        out_specs=jax.tree.map(lambda _: vmem, out_shape),
    )(x.reshape(1).astype(jnp.int32), *arrays)


def per_device(inputs, cotangent, up_weight, down_weight, norm_gain):
    width = inputs.shape[2]
    hid_width = up_weight.shape[1]
    x = lax.axis_index("tensor") // Z_COUNT
    section = lax.axis_index("section")
    in_rows = inputs.reshape(32, width)
    grad_rows = cotangent.reshape(32, width)

    both = lax.all_gather(
        jnp.concatenate([in_rows, grad_rows], axis=0), "section", axis=0, tiled=True
    ).reshape(SECTIONS, 64, width)
    per_chunk = SECTIONS // X_COUNT

    def chunk_of(value, k, start):
        index = ((x + k) % X_COUNT) * per_chunk
        return lax.dynamic_slice(value, (index, start, 0), (per_chunk, 32, width)).reshape(CHUNK, width)

    g_chunks = [chunk_of(both, k, 32) for k in range(X_COUNT)]

    def grad_hidden_part(k):
        return lax.dot_general(
            g_chunks[k], down_weight, (((1,), (1,)), ((), ())), preferred_element_type=f32
        ).astype(bf16)

    dh_parts = {k: grad_hidden_part(k) for k in (2, 1, 3)}

    a_all = both[:, :32].reshape(ROWS, width)
    a_stats = a_all.astype(f32)
    gain_rows = jnp.stack(split_three(norm_gain))
    gain_up = jnp.sum(jnp.dot(gain_rows, up_weight, preferred_element_type=f32), axis=0)
    row_parts = jnp.concatenate(
        [
            jnp.sum(a_stats, axis=1).reshape(4, 128),
            jnp.sum(a_stats * a_stats, axis=1).reshape(4, 128),
            gain_up.reshape(12, 128),
        ],
        axis=0,
    )
    dh_arrived = [shift_x(dh_parts[k], k) for k in (2, 1, 3)]
    summed = share(row_parts, "tensor")
    gain_up = summed[8:].reshape(hid_width)
    mean = (summed[:4] / D).reshape(ROWS)
    scale = lax.rsqrt((summed[4:8] / D).reshape(ROWS) - mean * mean + norm_eps)
    normed = ((a_all.astype(f32) - mean[:, None]) * scale[:, None] * norm_gain).astype(bf16)
    normed_three, g_chunks[0] = lax.optimization_barrier((normed.reshape(SECTIONS, 32, width), g_chunks[0]))
    line = lax.broadcasted_iota(jnp.int32, (ROWS, 128), 1)
    row_info = jnp.where(line == 0, mean[:, None], scale[:, None])
    normed_chunks = [chunk_of(normed_three, k, 0) for k in range(X_COUNT)]

    def pre_part(k):
        return jnp.dot(normed_chunks[k], up_weight, preferred_element_type=f32).astype(bf16)

    pre_arrived = [shift_x(pre_part(k), k) for k in (2, 1, 3)]
    pre_own = lax.optimization_barrier(pre_part(0))
    grad_hidden = reduce_chunks(grad_hidden_part(0), dh_arrived)
    pre = reduce_chunks(pre_own, pre_arrived)
    pre, row_info = lax.optimization_barrier((pre, row_info))
    grad_hidden = added(grad_hidden)
    pre = added(pre)

    hidden = gelu_tanh(pre).astype(bf16)
    grad_pre = (grad_hidden * gelu_slope(pre)).astype(bf16)
    grad_pre_float = grad_pre.astype(f32)
    terms = split_three(jnp.sum(grad_pre_float * gain_up, axis=1, keepdims=True))
    terms = terms + split_three(jnp.sum(grad_pre_float * pre, axis=1, keepdims=True))
    lane = lax.broadcasted_iota(jnp.int32, (16, EXTRA), 1)
    extra = jnp.zeros((16, EXTRA), bf16)
    for k, term in enumerate(terms):
        extra = jnp.where(lane == k, term, extra)

    grad_pre_own = spread_z(jnp.concatenate([grad_pre, extra], axis=1))
    hidden_own = spread_z(hidden)

    def gather_x(own):
        after = shift_x(own, -1)
        before = shift_x(own, 1)
        upper = shift_x(before[: CHUNK // 2], 1)
        lower = shift_x(after[CHUNK // 2 :], -1)
        return [own, after, upper, lower, before]

    wide_chunks = gather_x(grad_pre_own)
    hidden_chunks = gather_x(hidden_own)

    dx_part = on_device(
        input_grad_kernel,
        jax.ShapeDtypeStruct((SECTIONS, 32, width + 128), bf16),
        x,
        *wide_chunks,
        up_weight,
        both,
        row_info,
        norm_gain.reshape(1, width),
    )
    swapped = lax.all_to_all(dx_part, "section", 0, 0, tiled=True)
    own, after, upper, lower, before = hidden_chunks
    out_shape = jax.ShapeDtypeStruct((SECTIONS, 32, width), bf16)
    near = on_device(near_output_kernel, out_shape, x, own, after, before, down_weight)
    out_part = on_device(far_output_kernel, out_shape, x, upper, lower, near, down_weight)
    swapped_out = lax.all_to_all(out_part, "section", 0, 0, tiled=True)

    grad_up, grad_down = on_device(
        weight_grads_kernel,
        (
            jax.ShapeDtypeStruct((width, hid_width), bf16),
            jax.ShapeDtypeStruct((hid_width, width), bf16),
        ),
        x,
        *normed_chunks,
        *g_chunks,
        *wide_chunks,
        *hidden_chunks,
    )

    states = (in_rows.astype(f32) + added(swapped_out)).astype(bf16)
    own_scale = lax.dynamic_slice(row_info, (section * 32, 1), (32, 1))
    input_grads = (grad_rows.astype(f32) + own_scale * added(swapped[:, :, :width])).astype(bf16)
    lines = added(swapped[:, :16, width:])[:9]
    grad_gain = jnp.sum(lines.reshape(3, width), axis=0)
    return (
        states.reshape(inputs.shape),
        input_grads.reshape(inputs.shape),
        grad_up,
        grad_down,
        grad_gain,
    )


def solution(mesh):
    placed = (
        P(None, "section", "tensor"),
        P(None, "section", "tensor"),
        P("tensor", "section"),
        P("section", "tensor"),
        P("tensor"),
    )
    return jax.shard_map(
        per_device,
        mesh=mesh,
        in_specs=placed,
        out_specs=(
            P(None, "section", "tensor"),
            P(None, "section", "tensor"),
            P("tensor", "section"),
            P("section", "tensor"),
            P("tensor"),
        ),
        check_vma=False,
    )
```
